8 devices in a mesh: dp: 1 (over z), row: 2 (over y), col: 2 (over x), core: 2 (over core).
Axes of the slice: x: 2, y: 2, z: 1, core: 2. Of those that a mesh axis runs over, the one named last changes fastest.
Arguments:
- x: bfloat16 [1024, 896], P(('dp', 'row', 'col', 'core'))
- route_idx: int32 [1024, 8], P(('dp', 'row', 'col', 'core'))
- gates: float32 [1024, 8], P(('dp', 'row', 'col', 'core'))
- w1: bfloat16 [256, 896, 256], P(('row', 'col', 'core'))
- w3: bfloat16 [256, 896, 256], P(('row', 'col', 'core'))
- w2: bfloat16 [256, 256, 896], P(('row', 'col', 'core'))
- dy: bfloat16 [1024, 896], P(('dp', 'row', 'col', 'core'))
Outputs:
- output 1: bfloat16 [1024, 896], P(('dp', 'row', 'col', 'core'))
- output 2: bfloat16 [1024, 896], P(('dp', 'row', 'col', 'core'))
- output 3: float32 [1024, 8], P(('dp', 'row', 'col', 'core'))
- output 4: float32 [256, 896, 256], P(('dp', 'row', 'col', 'core'))
- output 5: float32 [256, 896, 256], P(('dp', 'row', 'col', 'core'))
- output 6: float32 [256, 256, 896], P(('dp', 'row', 'col', 'core'))
All inputs are finite; a program needn't handle non-finite values.
Results may differ from the reference program's by a relative error of at most 0.0104406.
Values are sent between devices in bfloat16 or wider.
A program may use at most 1 GiB of HBM per device.

```python
import jax
import jax.numpy as jnp
from jax import lax

TOKENS_DEV = 128
DEVICES = 8
DM = 896
FH = 256
EXPERTS = 256
TOP = 8
CAP = 10
TOKENS = TOKENS_DEV * DEVICES
GROUP_CAP = DEVICES * CAP


def _routes(key):
    half_td = TOKENS_DEV // 2
    half_e = EXPERTS // 2
    kr, ks, ka, kb = jax.random.split(jax.random.fold_in(key, 7), 4)
    ranks = jax.vmap(lambda k: jax.random.permutation(k, TOKENS_DEV))(jax.random.split(kr, DEVICES))
    sigma = jax.random.permutation(ks, EXPERTS)
    sa = jax.random.randint(ka, (), 0, half_e)
    sb = jax.random.randint(kb, (), 0, EXPERTS)
    devs = jnp.arange(DEVICES)[:, None] * half_td
    js = jnp.arange(TOP)
    ra = (ranks + devs + sa)[:, :, None] + (half_e // TOP) * js
    rb = (ranks - half_td + devs + sb)[:, :, None] + (EXPERTS // TOP) * js
    res = jnp.where((ranks < half_td)[:, :, None], ra % half_e, rb % EXPERTS)
    return sigma[res].reshape(TOKENS, TOP).astype(jnp.int32)


def setup_inputs(seed: int = 0, part: int = 0) -> dict:
    kp = jax.random.fold_in(jax.random.key(seed), part)
    kx, kr, kg, kd = jax.random.split(kp, 4)
    kw = jax.random.split(jax.random.key(seed + 1), 3)
    x = jax.random.normal(kx, (TOKENS, DM), jnp.float32).astype(jnp.bfloat16)
    route_idx = _routes(kr)
    gw = jax.random.uniform(kg, (TOKENS, TOP), jnp.float32, 0.5, 1.5)
    gates = 2.0 * gw / jnp.sum(gw, axis=1, keepdims=True)
    w1 = (jax.random.normal(kw[0], (EXPERTS, DM, FH), jnp.float32) * DM ** -0.5).astype(jnp.bfloat16)
    w3 = (jax.random.normal(kw[1], (EXPERTS, DM, FH), jnp.float32) * DM ** -0.5).astype(jnp.bfloat16)
    w2 = (jax.random.normal(kw[2], (EXPERTS, FH, DM), jnp.float32) * FH ** -0.5).astype(jnp.bfloat16)
    dy = jax.random.normal(kd, (TOKENS, DM), jnp.float32).astype(jnp.bfloat16)
    return {'x': x, 'route_idx': route_idx, 'gates': gates, 'w1': w1, 'w3': w3, 'w2': w2, 'dy': dy}


def _tables(route_idx):
    n = TOKENS * TOP
    e = route_idx.reshape(n)
    order = jnp.argsort(e, stable=True)
    counts = jnp.zeros((EXPERTS,), jnp.int32).at[e].add(1)
    starts = jnp.cumsum(counts) - counts
    c = jnp.arange(GROUP_CAP)
    pick = order[jnp.minimum(starts[:, None] + c[None, :], n - 1)]
    return jnp.where(c[None, :] < counts[:, None], pick, n)


def reference(x, route_idx, gates, w1, w3, w2, dy):
    n = TOKENS * TOP
    f32 = jnp.float32
    bf = jnp.bfloat16
    g_flat = gates.reshape(n)
    slot = _tables(route_idx)

    def expert(carry, inp):
        y_acc, dx_acc, dg = carry
        sl, a1, a3, a2 = inp
        tok = sl // TOP
        xr = jnp.take(x, tok, axis=0, mode='fill', fill_value=0)
        dyr = jnp.take(dy, tok, axis=0, mode='fill', fill_value=0)
        gr = jnp.take(g_flat, sl, mode='fill', fill_value=0)
        u = jnp.dot(xr, a1, preferred_element_type=f32).astype(bf)
        v = jnp.dot(xr, a3, preferred_element_type=f32).astype(bf)
        uf = u.astype(f32)
        vf = v.astype(f32)
        act = (jax.nn.silu(uf) * vf).astype(bf)
        o = jnp.dot(act, a2, preferred_element_type=f32).astype(bf)
        y_acc = y_acc.at[tok].add(gr[:, None] * o.astype(f32), mode='drop')
        dg = dg.at[sl].set(jnp.sum(dyr.astype(f32) * o.astype(f32), axis=1), mode='drop')
        dq = (gr[:, None] * dyr.astype(f32)).astype(bf)
        da = jnp.dot(dq, a2.T, preferred_element_type=f32).astype(bf)
        dw2 = jnp.dot(act.T, dq, preferred_element_type=f32)
        sg = jax.nn.sigmoid(uf)
        du = (da.astype(f32) * vf * sg * (1 + uf * (1 - sg))).astype(bf)
        dv = (da.astype(f32) * jax.nn.silu(uf)).astype(bf)
        dw1 = jnp.dot(xr.T, du, preferred_element_type=f32)
        dw3 = jnp.dot(xr.T, dv, preferred_element_type=f32)
        dxp = (jnp.dot(du, a1.T, preferred_element_type=f32) + jnp.dot(dv, a3.T, preferred_element_type=f32)).astype(bf)
        dx_acc = dx_acc.at[tok].add(dxp.astype(f32), mode='drop')
        return (y_acc, dx_acc, dg), (dw1, dw3, dw2)

    init = (jnp.zeros((TOKENS, DM), f32), jnp.zeros((TOKENS, DM), f32), jnp.zeros((n,), f32))
    (y_acc, dx_acc, dg), (dw1, dw3, dw2) = lax.scan(expert, init, (slot, w1, w3, w2))
    return (y_acc.astype(bf), dx_acc.astype(bf), dg.reshape(TOKENS, TOP), dw1, dw3, dw2)
```

```python
import functools

import jax
import jax.numpy as jnp
from jax import lax
from jax.experimental import pallas as pl
from jax.experimental.pallas import tpu as pltpu
from jax.sharding import PartitionSpec as P

MESH = pl.DeviceIdType.MESH
F32 = jnp.float32
BF = jnp.bfloat16
ROWS = 16
SLOTS = 5
DIM0 = (((0,), (0,)), ((), ()))
DIM1 = (((1,), (1,)), ((), ()))
ANY = pl.BlockSpec(memory_space=pl.ANY)


def _dot(a, b, dims=(((1,), (0,)), ((), ()))):
    return lax.dot_general(a, b, dims, preferred_element_type=F32)


def _core_kernel(x_hbm, dy_hbm, tab_hbm, w1_hbm, w3_hbm, w2_hbm,
                 xg_out, q_out, act_out, du_out, dv_out, y_out, dg_out, dx0, dx1, dx2, dx3,
                 x_all, dy_all, tab_all, xg, q, o, u, v, act, onehot, gate3,
                 w1, w3, w2, y_send, y_own, y_chip, y_far, d_send, d_own, d_chip, dg_send, dg_all, y_v, dg_v,
                 in_sem, w_sem, out_sem,
                 xs_sem, xr_sem, ys_sem, yr_sem, ts_sem, tr_sem,
                 yc_s, yc_r, yf_s, yf_r, dc_s, dc_r, gs_sem, gr_sem):
    row, col, core = lax.axis_index('row'), lax.axis_index('col'), lax.axis_index('core')
    el, dm, fh = w1_hbm.shape
    td = x_hbm.shape[0]
    top = tab_hbm.shape[0] // 2
    n_src = x_all.shape[0]

    def peer(k):
        r = 1 - row if k & 4 else row
        c = 1 - col if k & 2 else col
        h = 1 - core if k & 1 else core
        return {'row': r, 'col': c, 'core': h}, r * 4 + c * 2 + h

    me = peer(0)[1]

    own = [pltpu.make_async_copy(a, b.at[me], in_sem.at[i])
           for i, (a, b) in enumerate(((tab_hbm, tab_all), (x_hbm, x_all), (dy_hbm, dy_all)))]
    for c in own:
        c.start()

    def weights(i):
        e, slot = i % el, i % SLOTS
        return [pltpu.make_async_copy(a.at[e], b.at[slot], w_sem.at[j, slot])
                for j, (a, b) in enumerate(((w1_hbm, w1), (w3_hbm, w3), (w2_hbm, w2)))]

    for i in range(SLOTS):
        for c in weights(i):
            c.start()

    barrier = pltpu.get_barrier_semaphore()
    for k in range(1, n_src):
        pl.semaphore_signal(barrier, inc=1, device_id=peer(k)[0], device_id_type=MESH)
    pl.semaphore_wait(barrier, n_src - 1)

    def send(src, dst, s_sem, r_sem, k):
        c = pltpu.make_async_remote_copy(src_ref=src, dst_ref=dst, send_sem=s_sem, recv_sem=r_sem,
                                         device_id=peer(k)[0], device_id_type=MESH)
        c.start()
        return c

    def arrive(dst, s_sem, r_sem):
        pltpu.make_async_remote_copy(src_ref=dst, dst_ref=dst, send_sem=s_sem, recv_sem=r_sem,
                                     device_id=peer(1)[0], device_id_type=MESH).wait_recv()

    sent = []
    own[0].wait()
    for k in range(1, n_src):
        sent.append(send(tab_all.at[me], tab_all.at[me], ts_sem.at[k], tr_sem.at[me], k))
    own[1].wait()
    for k in (2, 4, 6, 1):
        sent.append(send(x_all.at[me], x_all.at[me], xs_sem.at[k], xr_sem.at[me], k))
    own[2].wait()
    for k in (2, 4, 6, 1):
        sent.append(send(dy_all.at[me], dy_all.at[me], ys_sem.at[k], yr_sem.at[me], k))

    for k in range(1, n_src):
        s = peer(k)[1]
        arrive(tab_all.at[s], ts_sem.at[k], tr_sem.at[s])

    experts = (lax.broadcasted_iota(jnp.int32, (el, td), 0) + me * el).astype(F32)
    before = (lax.broadcasted_iota(jnp.int32, (td, td), 0) < lax.broadcasted_iota(jnp.int32, (td, td), 1))
    before = jnp.where(before, 1.0, 0.0).astype(BF)
    place = lax.broadcasted_iota(jnp.int32, (el, ROWS, td), 1).astype(F32)

    def tables(s, _):
        hit = jnp.zeros((el, td), F32)
        gate = jnp.zeros((el, td), F32)
        for j in range(top):
            m = tab_all[s, j:j + 1, :] == experts
            hit = jnp.where(m, 1.0, hit)
            gate = jnp.where(m, tab_all[s, top + j:top + j + 1, :], gate)
        rank = _dot(hit.astype(BF), before)
        rank = jnp.where(hit > 0, rank, -1.0)
        sel = jnp.broadcast_to(rank[:, None, :], place.shape) == place
        onehot[s] = jnp.where(sel, 1.0, 0.0).astype(BF).reshape(el * ROWS, td)
        g = jnp.where(sel, jnp.broadcast_to(gate[:, None, :], place.shape), 0.0).reshape(el * ROWS, td)
        for i in range(3):
            part = g.astype(BF)
            gate3[s, :, i * td:(i + 1) * td] = part
            g = g - part.astype(F32)
        return 0

    lax.fori_loop(0, n_src, tables, 0)

    def rows_of(s):
        return pl.ds(pl.multiple_of(s * ROWS, ROWS), ROWS)

    for k in (0, 1, 2, 4, 6, 3, 5, 7):
        s = peer(k)[1]
        if k:
            arrive(x_all.at[s], xs_sem.at[k], xr_sem.at[s])
        if k in (2, 4, 6):
            sent.append(send(x_all.at[s], x_all.at[s], xs_sem.at[k + 1], xr_sem.at[s], 1))
        xg[:, rows_of(s), :] = _dot(onehot[s], x_all[s]).astype(BF).reshape(el, ROWS, dm)
    outs = [pltpu.make_async_copy(xg, xg_out, out_sem.at[0])]
    outs[0].start()

    def forward(e, _):
        slot = e % SLOTS
        for c in weights(e):
            c.wait()
        xe = xg[e]
        ue = _dot(xe, w1[slot]).astype(BF)
        ve = _dot(xe, w3[slot]).astype(BF)
        u[e] = ue
        v[e] = ve
        uf = ue.astype(F32)
        a = (uf * jax.nn.sigmoid(uf) * ve.astype(F32)).astype(BF)
        act[e] = a
        o[e] = _dot(a, w2[slot]).astype(BF)
        for c in weights(e + SLOTS):
            c.start()
        return 0

    half = el // 2
    lax.fori_loop(0, half, forward, 0)
    for k in (2, 4, 6):
        s = peer(k)[1]
        arrive(dy_all.at[s], ys_sem.at[k], yr_sem.at[s])
        sent.append(send(dy_all.at[s], dy_all.at[s], ys_sem.at[k + 1], yr_sem.at[s], 1))
    lax.fori_loop(half, el, forward, 0)
    outs.append(pltpu.make_async_copy(act, act_out, out_sem.at[1]))
    outs[1].start()

    def y_part(s):
        z = _dot(gate3[s], o[:, rows_of(s), :].reshape(el * ROWS, dm), DIM0)
        return z[:td] + z[td:2 * td] + z[2 * td:]

    for j in range(4):
        y_send[j] = y_part(peer(2 * j + 1)[1])
        sent.append(send(y_send.at[j], y_chip.at[j], yc_s.at[j], yc_r.at[j], 1))
    for j in range(4):
        y_own[j] = y_part(peer(2 * j)[1])
    for j in (3, 1, 2, 0):
        arrive(y_chip.at[j], yc_s.at[j], yc_r.at[j])
        y_own[j] = y_own[j] + y_chip[j]
        if j:
            sent.append(send(y_own.at[j], y_far.at[j - 1], yf_s.at[j - 1], yf_r.at[j - 1], 2 * j))

    def dispatch_dy(s, k):
        d = _dot(onehot[s], dy_all[s])
        os = o[:, rows_of(s), :].reshape(el * ROWS, dm).astype(F32)
        hot = onehot[s].astype(F32)
        dg = jnp.sum(d * os, axis=1, keepdims=True)
        dgt = jnp.sum((hot * dg).reshape(el, ROWS, td), axis=1)
        g = gate3[s]
        g = g[:, :td].astype(F32) + g[:, td:2 * td].astype(F32) + g[:, 2 * td:].astype(F32)
        g = jnp.sum(g, axis=1, keepdims=True)
        q[:, rows_of(s), :] = (g * d).astype(BF).reshape(el, ROWS, dm)
        for j in range(top):
            m = tab_all[s, j:j + 1, :] == experts
            dg_send[s, j:j + 1, :] = jnp.sum(jnp.where(m, dgt, 0.0), axis=0, keepdims=True)

    for k in (0, 1, 2, 4, 6, 3, 5, 7):
        s = peer(k)[1]
        if k in (1, 3, 5, 7):
            arrive(dy_all.at[s], ys_sem.at[k], yr_sem.at[s])
        dispatch_dy(s, k)
        if k:
            sent.append(send(dg_send.at[s], dg_all.at[me], gs_sem.at[k], gr_sem.at[me], k))
        else:
            dg_all[me] = dg_send[s]
    outs.append(pltpu.make_async_copy(q, q_out, out_sem.at[2]))
    outs[2].start()

    def backward(i, _):
        e = i - el
        slot = i % SLOTS
        for c in weights(i):
            c.wait()
        da = _dot(q[e], w2[slot], DIM1).astype(BF).astype(F32)
        uf = u[e].astype(F32)
        vf = v[e].astype(F32)
        sg = jax.nn.sigmoid(uf)
        du = (da * vf * sg * (1 + uf * (1 - sg))).astype(BF)
        dv = (da * (uf * sg)).astype(BF)
        u[e] = du
        v[e] = dv
        o[e] = (_dot(du, w1[slot], DIM1) + _dot(dv, w3[slot], DIM1)).astype(BF)

        @pl.when(i + SLOTS < 2 * el)
        def _():
            for c in weights(i + SLOTS):
                c.start()
        return 0

    lax.fori_loop(el, 2 * el, backward, 0)
    for i, (a, b) in enumerate(((u, du_out), (v, dv_out))):
        outs.append(pltpu.make_async_copy(a, b, out_sem.at[3 + i]))
        outs[-1].start()

    def dx_part(s):
        return _dot(onehot[s], o[:, rows_of(s), :].reshape(el * ROWS, dm), DIM0)

    for j in range(4):
        d_send[j] = dx_part(peer(2 * j + 1)[1])
        sent.append(send(d_send.at[j], d_chip.at[j], dc_s.at[j], dc_r.at[j], 1))
    for j in range(4):
        d_own[j] = dx_part(peer(2 * j)[1])

    for j in range(3):
        arrive(y_far.at[j], yf_s.at[j], yf_r.at[j])
    y_v[...] = (y_own[0] + y_far[0] + y_far[1] + y_far[2]).astype(BF)
    for k in range(1, n_src):
        s = peer(k)[1]
        arrive(dg_all.at[s], gs_sem.at[k], gr_sem.at[s])
    dg_v[...] = jnp.sum(dg_all[...], axis=0)
    outs.append(pltpu.make_async_copy(y_v, y_out, out_sem.at[5]))
    outs[-1].start()
    outs.append(pltpu.make_async_copy(dg_v, dg_out, out_sem.at[6]))
    outs[-1].start()

    for j, out in ((3, dx3), (1, dx1), (2, dx2), (0, dx0)):
        arrive(d_chip.at[j], dc_s.at[j], dc_r.at[j])
        d_own[j] = d_own[j] + d_chip[j]
        outs.append(pltpu.make_async_copy(d_own.at[j], out, out_sem.at[7 + j]))
        outs[-1].start()

    for c in sent:
        c.wait_send()
    for c in outs:
        c.wait()


def _grad_kernel(xg, q, act, du, dv, dw1, dw3, dw2):
    for i in range(xg.shape[0]):
        dw1[i] = _dot(xg[i], du[i], DIM0)
        dw3[i] = _dot(xg[i], dv[i], DIM0)
        dw2[i] = _dot(act[i], q[i], DIM0)


def solution(mesh):
    ep = ('row', 'col', 'core')
    n_src = mesh.shape['row'] * mesh.shape['col'] * mesh.shape['core']
    tspec = P(('dp',) + ep, None)
    wspec = P(ep, None, None)
    gspec = P(('dp',) + ep, None, None)

    def body(x, route_idx, gates, w1, w3, w2, dy):
        td, top = route_idx.shape
        el, dm, fh = w1.shape
        er = n_src * ROWS
        tab = jnp.concatenate([route_idx.T.astype(F32), gates.T], axis=0)
        sds = jax.ShapeDtypeStruct
        dma = pltpu.SemaphoreType.DMA
        block = (td, dm)
        flops = 2 * el * er * dm * fh * 6
        xg, q, act, du, dv, y, dg, dx0, dx1, dx2, dx3 = pl.pallas_call(
            _core_kernel,
            name='moe_core',
            out_shape=[sds((el, er, dm), BF), sds((el, er, dm), BF)] + [sds((el, er, fh), BF)] * 3
            + [sds(block, BF), sds((top, td), F32)] + [sds(block, F32)] * 4,
            in_specs=[ANY] * 6,
            out_specs=[ANY] * 11,
            scratch_shapes=[
                pltpu.VMEM((n_src,) + block, BF), pltpu.VMEM((n_src,) + block, BF), pltpu.VMEM((n_src, 2 * top, td), F32),
                pltpu.VMEM((el, er, dm), BF), pltpu.VMEM((el, er, dm), BF), pltpu.VMEM((el, er, dm), BF),
                pltpu.VMEM((el, er, fh), BF), pltpu.VMEM((el, er, fh), BF), pltpu.VMEM((el, er, fh), BF),
                pltpu.VMEM((n_src, el * ROWS, td), BF), pltpu.VMEM((n_src, el * ROWS, 3 * td), BF),
                pltpu.VMEM((SLOTS, dm, fh), BF), pltpu.VMEM((SLOTS, dm, fh), BF), pltpu.VMEM((SLOTS, fh, dm), BF),
                pltpu.VMEM((4,) + block, F32), pltpu.VMEM((4,) + block, F32), pltpu.VMEM((4,) + block, F32),
                pltpu.VMEM((3,) + block, F32),
                pltpu.VMEM((4,) + block, F32), pltpu.VMEM((4,) + block, F32), pltpu.VMEM((4,) + block, F32),
                pltpu.VMEM((n_src, top, td), F32), pltpu.VMEM((n_src, top, td), F32),
                pltpu.VMEM(block, BF), pltpu.VMEM((top, td), F32),
                dma((3,)), dma((3, SLOTS)), dma((11,)),
                dma((8,)), dma((8,)), dma((8,)), dma((8,)), dma((8,)), dma((8,)),
                dma((4,)), dma((4,)), dma((3,)), dma((3,)), dma((4,)), dma((4,)), dma((8,)), dma((8,)),
            ],
            compiler_params=pltpu.CompilerParams(collective_id=0, has_side_effects=True, vmem_limit_bytes=67043328),
            cost_estimate=pl.CostEstimate(flops=flops, bytes_accessed=88 << 20, transcendentals=0),
        )(x, dy, tab, w1, w3, w2)

        def swap(a, k):
            return lax.ppermute(a, ep, [(i, i ^ k) for i in range(n_src)])

        far = [swap(dx3, 6), swap(dx1, 2), swap(dx2, 4)]
        per = 2
        spec = lambda a, b: pl.BlockSpec((per, a, b), lambda i: (i, 0, 0))
        dw1, dw3, dw2 = pl.pallas_call(
            _grad_kernel,
            name='moe_grad',
            grid=(el // per,),
            out_shape=[sds((el, dm, fh), F32), sds((el, dm, fh), F32), sds((el, fh, dm), F32)],
            in_specs=[spec(er, dm), spec(er, dm), spec(er, fh), spec(er, fh), spec(er, fh)],
            out_specs=[spec(dm, fh), spec(dm, fh), spec(fh, dm)],
            compiler_params=pltpu.CompilerParams(vmem_limit_bytes=62 << 20),
            cost_estimate=pl.CostEstimate(flops=2 * el * er * dm * fh * 3, bytes_accessed=110 << 20, transcendentals=0),
        )(xg, q, act, du, dv)
        dx = (dx0 + far[0] + far[1] + far[2]).astype(BF)
        return y, dx, dg.T, dw1, dw3, dw2

    return jax.shard_map(body, mesh=mesh, in_specs=(tspec, tspec, tspec, wspec, wspec, wspec, tspec),
                         out_specs=(tspec, tspec, tspec, gspec, gspec, gspec), check_vma=False)
```

```python
import functools

import jax
import jax.numpy as jnp
from jax import lax
from jax.experimental import pallas as pl
from jax.experimental.pallas import tpu as pltpu
from jax.sharding import PartitionSpec as P

MESH = pl.DeviceIdType.MESH
F32 = jnp.float32
BF = jnp.bfloat16
ROWS = 16
SLOTS = 12
CORE_VMEM = 43
GRAD_VMEM = 14
GROUP = 2
DIM0 = (((0,), (0,)), ((), ()))
DIM1 = (((1,), (1,)), ((), ()))
ANY = pl.BlockSpec(memory_space=pl.ANY)


def _dot(a, b, dims=(((1,), (0,)), ((), ()))):
    return lax.dot_general(a, b, dims, preferred_element_type=F32)


def _core_kernel(x_hbm, dy_hbm, route_hbm, gate_hbm, w1_hbm, w3_hbm, w2_hbm,
                 xg, q, act, u, v, y_out, dg_out, dx0, dx1, dx2, dx3,
                 x_all, dy_all, route_all, gate_all, o, onehot, onehot_t, gate3_t,
                 w1, w3, w2, y_send, y_own, y_chip, y_far, d_own, dg_send, dg_all,
                 in_sem, w_sem, out_sem,
                 xs_sem, xr_sem, ys_sem, yr_sem, ts_sem, tr_sem, gts_sem, gtr_sem,
                 yc_s, yc_r, yf_s, yf_r, dc_s, dc_r, gs_sem, gr_sem):
    row, col, core = lax.axis_index('row'), lax.axis_index('col'), lax.axis_index('core')
    el, dm, fh = w1_hbm.shape
    td = x_hbm.shape[0]
    top = route_hbm.shape[0]
    n_src = x_all.shape[0]

    def peer(k):
        r = 1 - row if k & 4 else row
        c = 1 - col if k & 2 else col
        h = 1 - core if k & 1 else core
        return {'row': r, 'col': c, 'core': h}, r * 4 + c * 2 + h

    me = peer(0)[1]

    def start(copies):
        for c in copies:
            c.start()

    def wait(copies):
        for c in copies:
            c.wait()

    own = [pltpu.make_async_copy(a, b.at[me], in_sem.at[i])
           for i, (a, b) in enumerate(((route_hbm, route_all), (gate_hbm, gate_all), (x_hbm, x_all), (dy_hbm, dy_all)))]
    start(own)

    def up(e):
        slot = e % SLOTS
        return [pltpu.make_async_copy(a.at[e], b.at[slot], w_sem.at[j, slot])
                for j, (a, b) in enumerate(((w1_hbm, w1), (w3_hbm, w3)))]

    def down(e):
        return [pltpu.make_async_copy(w2_hbm.at[e], w2.at[e % SLOTS], w_sem.at[2, e % SLOTS])]

    barrier = pltpu.get_barrier_semaphore()
    for k in range(1, n_src):
        pl.semaphore_signal(barrier, inc=1, device_id=peer(k)[0], device_id_type=MESH)
    for e in range(SLOTS):
        start(up(e) + down(e))
    pl.semaphore_wait(barrier, n_src - 1)

    def send(src, dst, s_sem, r_sem, k):
        c = pltpu.make_async_remote_copy(src_ref=src, dst_ref=dst, send_sem=s_sem, recv_sem=r_sem,
                                         device_id=peer(k)[0], device_id_type=MESH)
        c.start()
        return c

    def arrive(dst, s_sem, r_sem):
        pltpu.make_async_remote_copy(src_ref=dst, dst_ref=dst, send_sem=s_sem, recv_sem=r_sem,
                                     device_id=peer(1)[0], device_id_type=MESH).wait_recv()

    sent = []
    wait(own[:2])
    for k in range(1, n_src):
        sent.append(send(route_all.at[me], route_all.at[me], ts_sem.at[k], tr_sem.at[me], k))
        sent.append(send(gate_all.at[me], gate_all.at[me], gts_sem.at[k], gtr_sem.at[me], k))
    wait(own[2:])
    for k in (2, 4, 6, 1):
        sent.append(send(x_all.at[me], x_all.at[me], xs_sem.at[k], xr_sem.at[me], k))

    for k in range(1, n_src):
        s = peer(k)[1]
        arrive(route_all.at[s], ts_sem.at[k], tr_sem.at[s])
        arrive(gate_all.at[s], gts_sem.at[k], gtr_sem.at[s])

    experts = lax.broadcasted_iota(jnp.int32, (el, td), 0) + me * el
    before = (lax.broadcasted_iota(jnp.int32, (td, td), 0) < lax.broadcasted_iota(jnp.int32, (td, td), 1))
    before = jnp.where(before, 1.0, 0.0).astype(BF)
    place = lax.broadcasted_iota(jnp.int32, (el, ROWS, td), 1).astype(F32)

    def gates_of(s):
        gate = jnp.zeros((el, td), F32)
        for j in range(top):
            gate = jnp.where(route_all[s, j:j + 1, :] == experts, gate_all[s, j:j + 1, :], gate)
        return gate

    def tables(s, _):
        hit = jnp.zeros((el, td), F32)
        for j in range(top):
            hit = jnp.where(route_all[s, j:j + 1, :] == experts, 1.0, hit)
        rank = jnp.where(hit > 0, _dot(hit.astype(BF), before), -1.0)
        sel = jnp.broadcast_to(rank[:, None, :], place.shape) == place
        hot = jnp.where(sel, 1.0, 0.0).reshape(el * ROWS, td)
        onehot[s] = hot.astype(BF)
        onehot_t[s] = hot.T.astype(BF)
        g = jnp.where(sel, jnp.broadcast_to(gates_of(s)[:, None, :], place.shape), 0.0)
        g = g.reshape(el * ROWS, td).T
        for i in range(3):
            part = g.astype(BF)
            gate3_t[s, i * td:(i + 1) * td, :] = part
            g = g - part.astype(F32)
        return 0

    lax.fori_loop(0, n_src, tables, 0)

    def rows_of(s):
        return pl.ds(pl.multiple_of(s * ROWS, ROWS), ROWS)

    for k in (0, 1, 2, 4, 6, 3, 5, 7):
        s = peer(k)[1]
        if k:
            arrive(x_all.at[s], xs_sem.at[k], xr_sem.at[s])
        if k in (2, 4, 6):
            sent.append(send(x_all.at[s], x_all.at[s], xs_sem.at[k + 1], xr_sem.at[s], 1))
        if k == 6:
            for j in (2, 4, 6, 1):
                sent.append(send(dy_all.at[me], dy_all.at[me], ys_sem.at[j], yr_sem.at[me], j))
        xg[:, rows_of(s), :] = _dot(onehot[s], x_all[s]).astype(BF).reshape(el, ROWS, dm)

    def group(p):
        return [p * GROUP + i for i in range(GROUP)]

    groups = el // GROUP

    def forward_hidden(e):
        slot = e % SLOTS
        xe = xg[e]
        ue = _dot(xe, w1[slot]).astype(BF)
        ve = _dot(xe, w3[slot]).astype(BF)
        u[e] = ue
        v[e] = ve
        uf = ue.astype(F32)
        act[e] = (uf * jax.nn.sigmoid(uf) * ve.astype(F32)).astype(BF)

    def forward_out(e):
        o[e] = _dot(act[e], w2[e % SLOTS]).astype(BF)

    def ahead(copies, es):
        for e in es:
            @pl.when(e + SLOTS < el)
            def _():
                start(copies(e + SLOTS))

    def forward(p, _):
        prev, now = group(p - 1), group(p)
        for e in prev:
            wait(down(e))
        for e in now:
            wait(up(e))
        for e in prev:
            forward_out(e)
        for e in now:
            forward_hidden(e)
        ahead(down, prev)
        ahead(up, now)
        return 0

    for e in group(0):
        wait(up(e))
    for e in group(0):
        forward_hidden(e)
    for e in group(0):
        start(up(e + SLOTS))
    lax.fori_loop(1, groups, forward, 0)
    for e in group(groups - 1):
        wait(down(e))
    for e in group(groups - 1):
        forward_out(e)

    def y_part(s):
        z = _dot(gate3_t[s], o[:, rows_of(s), :].reshape(el * ROWS, dm))
        return z[:td] + z[td:2 * td] + z[2 * td:]

    chip = []
    for j in range(4):
        y_send[j] = y_part(peer(2 * j + 1)[1])
        chip.append(send(y_send.at[j], y_chip.at[j], yc_s.at[j], yc_r.at[j], 1))
    for k in (2, 4, 6):
        s = peer(k)[1]
        arrive(dy_all.at[s], ys_sem.at[k], yr_sem.at[s])
        sent.append(send(dy_all.at[s], dy_all.at[s], ys_sem.at[k + 1], yr_sem.at[s], 1))
    for j in range(4):
        y_own[j] = y_part(peer(2 * j)[1])
    for j in (3, 1, 2, 0):
        arrive(y_chip.at[j], yc_s.at[j], yc_r.at[j])
        y_own[j] = y_own[j] + y_chip[j]
        if j:
            sent.append(send(y_own.at[j], y_far.at[j - 1], yf_s.at[j - 1], yf_r.at[j - 1], 2 * j))

    def dispatch_dy(s):
        gate = gates_of(s)
        dgt = []
        part = el // 4
        for h in range(4):
            es = slice(h * part, (h + 1) * part)
            hot = onehot[s, h * part * ROWS:(h + 1) * part * ROWS, :]
            d = _dot(hot, dy_all[s])
            hot = hot.astype(F32)
            os = o[es, rows_of(s), :].reshape(part * ROWS, dm).astype(F32)
            dg = jnp.sum(d * os, axis=1, keepdims=True)
            dgt.append(jnp.sum((hot * dg).reshape(part, ROWS, td), axis=1))
            g = jnp.broadcast_to(gate[es][:, None, :], (part, ROWS, td)).reshape(part * ROWS, td)
            g = jnp.sum(hot * g, axis=1, keepdims=True)
            q[es, rows_of(s), :] = (g * d).astype(BF).reshape(part, ROWS, dm)
        dgt = jnp.concatenate(dgt, axis=0)
        for j in range(top):
            m = route_all[s, j:j + 1, :] == experts
            dg_send[s, j:j + 1, :] = jnp.sum(jnp.where(m, dgt, 0.0), axis=0, keepdims=True)

    for k in (0, 1, 2, 4, 6, 3, 5, 7):
        s = peer(k)[1]
        if k in (1, 3, 5, 7):
            arrive(dy_all.at[s], ys_sem.at[k], yr_sem.at[s])
        dispatch_dy(s)
        if k:
            sent.append(send(dg_send.at[s], dg_all.at[me], gs_sem.at[k], gr_sem.at[me], k))
        else:
            dg_all[me] = dg_send[s]

    def backward_hidden(e):
        da = _dot(q[e], w2[e % SLOTS], DIM1).astype(BF).astype(F32)
        uf = u[e].astype(F32)
        vf = v[e].astype(F32)
        sg = jax.nn.sigmoid(uf)
        u[e] = (da * vf * sg * (1 + uf * (1 - sg))).astype(BF)
        v[e] = (da * (uf * sg)).astype(BF)

    def backward_out(e):
        slot = e % SLOTS
        o[e] = (_dot(u[e], w1[slot], DIM1) + _dot(v[e], w3[slot], DIM1)).astype(BF)

    def refill(copies, es):
        for e in es:
            @pl.when(e >= SLOTS)
            def _():
                start(copies(e - SLOTS))

    def ready(copies, es):
        for e in es:
            @pl.when(e < el - SLOTS)
            def _():
                wait(copies(e))

    def down_group(p):
        return [el - 1 - (p * GROUP + i) for i in range(GROUP)]

    def backward(p, _):
        prev, now = down_group(p - 1), down_group(p)
        ready(up, prev)
        ready(down, now)
        for e in prev:
            backward_out(e)
        for e in now:
            backward_hidden(e)
        refill(up, prev)
        refill(down, now)
        return 0

    for e in down_group(0):
        backward_hidden(e)
    refill(down, down_group(0))
    lax.fori_loop(1, groups, backward, 0)
    ready(up, down_group(groups - 1))
    for e in down_group(groups - 1):
        backward_out(e)

    for k in range(1, n_src):
        s = peer(k)[1]
        arrive(dg_all.at[s], gs_sem.at[k], gr_sem.at[s])
    for c in chip:
        c.wait_send()

    def dx_part(s):
        return _dot(onehot_t[s], o[:, rows_of(s), :].reshape(el * ROWS, dm))

    for j in range(4):
        y_send[j] = dx_part(peer(2 * j + 1)[1])
        sent.append(send(y_send.at[j], y_chip.at[j], dc_s.at[j], dc_r.at[j], 1))
    for j in range(4):
        d_own[j] = dx_part(peer(2 * j)[1])
    outs = []
    for j, out in ((3, dx3), (1, dx1), (2, dx2), (0, dx0)):
        arrive(y_chip.at[j], dc_s.at[j], dc_r.at[j])
        d_own[j] = d_own[j] + y_chip[j]
        outs.append(pltpu.make_async_copy(d_own.at[j], out, out_sem.at[j]))
        outs[-1].start()

    for j in range(3):
        arrive(y_far.at[j], yf_s.at[j], yf_r.at[j])
    y_out[...] = (y_own[0] + y_far[0] + y_far[1] + y_far[2]).astype(BF)
    dg_out[...] = jnp.sum(dg_all[...], axis=0)

    for c in sent:
        c.wait_send()
    wait(outs)


def _grad_kernel(xg, q, act, du, dv, y, dg, dw1, dw3, dw2, y_out, dg_out):
    for i in range(xg.shape[0]):
        dw1[i] = _dot(xg[i], du[i], DIM0)
        dw3[i] = _dot(xg[i], dv[i], DIM0)
        dw2[i] = _dot(act[i], q[i], DIM0)
    y_out[...] = y[...]
    dg_out[...] = dg[...]


def solution(mesh):
    ep = ('row', 'col', 'core')
    n_src = mesh.shape['row'] * mesh.shape['col'] * mesh.shape['core']
    tspec = P(('dp',) + ep, None)
    wspec = P(ep, None, None)
    gspec = P(('dp',) + ep, None, None)

    def body(x, route_idx, gates, w1, w3, w2, dy):
        td, top = route_idx.shape
        el, dm, fh = w1.shape
        er = n_src * ROWS
        sds = jax.ShapeDtypeStruct
        vmem = pltpu.VMEM
        dma = pltpu.SemaphoreType.DMA
        block = (td, dm)
        small = (n_src, top, td)
        whole = pl.BlockSpec(memory_space=pltpu.VMEM)
        flops = 2 * el * er * dm * fh * 6
        xg, q, act, du, dv, y, dg, dx0, dx1, dx2, dx3 = pl.pallas_call(
            _core_kernel,
            name='moe_core',
            out_shape=[vmem((el, er, dm), BF), vmem((el, er, dm), BF)] + [vmem((el, er, fh), BF)] * 3
            + [vmem(block, BF), vmem((top, td), F32)] + [sds(block, F32)] * 4,
            in_specs=[ANY] * 7,
            out_specs=[whole] * 7 + [ANY] * 4,
            scratch_shapes=[
                vmem((n_src,) + block, BF), vmem((n_src,) + block, BF), vmem(small, jnp.int32), vmem(small, F32),
                vmem((el, er, dm), BF),
                vmem((n_src, el * ROWS, td), BF), vmem((n_src, td, el * ROWS), BF), vmem((n_src, 3 * td, el * ROWS), BF),
                vmem((SLOTS, dm, fh), BF), vmem((SLOTS, dm, fh), BF), vmem((SLOTS, fh, dm), BF),
                vmem((4,) + block, F32), vmem((4,) + block, F32), vmem((4,) + block, F32), vmem((3,) + block, F32),
                vmem((4,) + block, F32), vmem(small, F32), vmem(small, F32),
                dma((4,)), dma((3, SLOTS)), dma((4,)),
                dma((8,)), dma((8,)), dma((8,)), dma((8,)), dma((8,)), dma((8,)), dma((8,)), dma((8,)),
                dma((4,)), dma((4,)), dma((3,)), dma((3,)), dma((4,)), dma((4,)), dma((8,)), dma((8,)),
            ],
            compiler_params=pltpu.CompilerParams(collective_id=0, has_side_effects=True, vmem_limit_bytes=CORE_VMEM << 20),
            cost_estimate=pl.CostEstimate(flops=flops, bytes_accessed=88 << 20, transcendentals=0),
        )(x, dy, route_idx.T, gates.T, w1, w3, w2)

        def swap(a, k):
            return lax.ppermute(a, ep, [(i, i ^ k) for i in range(n_src)])

        far = [swap(dx3, 6), swap(dx1, 2), swap(dx2, 4)]
        per = 2
        spec = lambda a, b: pl.BlockSpec((per, a, b), lambda i: (i, 0, 0))
        once = lambda a, b: pl.BlockSpec((a, b), lambda i: (0, 0))

        dw1, dw3, dw2, y, dg = pl.pallas_call(
            _grad_kernel,
            name='moe_grad',
            grid=(el // per,),
            out_shape=[sds((el, dm, fh), F32), sds((el, dm, fh), F32), sds((el, fh, dm), F32), sds(block, BF), sds((top, td), F32)],
            in_specs=[spec(er, dm), spec(er, dm), spec(er, fh), spec(er, fh), spec(er, fh), once(td, dm), once(top, td)],
            out_specs=[spec(dm, fh), spec(dm, fh), spec(fh, dm), once(td, dm), once(top, td)],
            compiler_params=pltpu.CompilerParams(vmem_limit_bytes=GRAD_VMEM << 20),
            cost_estimate=pl.CostEstimate(flops=2 * el * er * dm * fh * 3, bytes_accessed=90 << 20, transcendentals=0),
        )(xg, q, act, du, dv, y, dg)
        dx = (dx0 + far[0] + far[1] + far[2]).astype(BF)
        return y, dx, dg.T, dw1, dw3, dw2

    return jax.shard_map(body, mesh=mesh, in_specs=(tspec, tspec, tspec, wspec, wspec, wspec, tspec),
                         out_specs=(tspec, tspec, tspec, gspec, gspec, gspec), check_vma=False)
```

```python
import functools

import jax
import jax.numpy as jnp
from jax import lax
from jax.experimental import pallas as pl
from jax.experimental.pallas import tpu as pltpu
from jax.sharding import PartitionSpec as P

MESH = pl.DeviceIdType.MESH
F32 = jnp.float32
BF = jnp.bfloat16
ROWS = 16
SLOTS = 12
FORWARD_AT = 4
CORE_VMEM = 43
GRAD_VMEM = 14
GROUP = 4
DIM0 = (((0,), (0,)), ((), ()))
DIM1 = (((1,), (1,)), ((), ()))
ANY = pl.BlockSpec(memory_space=pl.ANY)


def _dot(a, b, dims=(((1,), (0,)), ((), ()))):
    return lax.dot_general(a, b, dims, preferred_element_type=F32)


def _core_kernel(x_hbm, dy_hbm, route_hbm, gate_hbm, w1_hbm, w3_hbm, w2_hbm,
                 xg, q, act, u, v, y_out, dg_out, dx0, dx1, dx2, dx3,
                 x_all, dy_all, route_all, gate_all, o, onehot, onehot_t, gate3_t,
                 w1, w3, w2, y_send, y_own, y_chip, y_far, d_own, dg_send, dg_all,
                 in_sem, w_sem, out_sem,
                 xs_sem, xr_sem, ys_sem, yr_sem, ts_sem, tr_sem, gts_sem, gtr_sem,
                 yc_s, yc_r, yf_s, yf_r, dc_s, dc_r, gs_sem, gr_sem):
    row, col, core = lax.axis_index('row'), lax.axis_index('col'), lax.axis_index('core')
    el, dm, fh = w1_hbm.shape
    td = x_hbm.shape[0]
    top = route_hbm.shape[0]
    n_src = x_all.shape[0]

    def peer(k):
        r = 1 - row if k & 4 else row
        c = 1 - col if k & 2 else col
        h = 1 - core if k & 1 else core
        return {'row': r, 'col': c, 'core': h}, r * 4 + c * 2 + h

    me = peer(0)[1]

    def start(copies):
        for c in copies:
            c.start()

    def wait(copies):
        for c in copies:
            c.wait()

    own = [pltpu.make_async_copy(a, b.at[me], in_sem.at[i])
           for i, (a, b) in enumerate(((route_hbm, route_all), (gate_hbm, gate_all), (x_hbm, x_all), (dy_hbm, dy_all)))]
    start(own)

    def up(e):
        slot = e % SLOTS
        return [pltpu.make_async_copy(a.at[e], b.at[slot], w_sem.at[j, slot])
                for j, (a, b) in enumerate(((w1_hbm, w1), (w3_hbm, w3)))]

    def down(e):
        return [pltpu.make_async_copy(w2_hbm.at[e], w2.at[e % SLOTS], w_sem.at[2, e % SLOTS])]

    barrier = pltpu.get_barrier_semaphore()
    for k in range(1, n_src):
        pl.semaphore_signal(barrier, inc=1, device_id=peer(k)[0], device_id_type=MESH)
    for e in range(SLOTS):
        start(up(e) + down(e))
    pl.semaphore_wait(barrier, n_src - 1)

    def send(src, dst, s_sem, r_sem, k):
        c = pltpu.make_async_remote_copy(src_ref=src, dst_ref=dst, send_sem=s_sem, recv_sem=r_sem,
                                         device_id=peer(k)[0], device_id_type=MESH)
        c.start()
        return c

    def arrive(dst, s_sem, r_sem):
        pltpu.make_async_remote_copy(src_ref=dst, dst_ref=dst, send_sem=s_sem, recv_sem=r_sem,
                                     device_id=peer(1)[0], device_id_type=MESH).wait_recv()

    sent = []
    wait(own[:2])
    for k in range(1, n_src):
        sent.append(send(route_all.at[me], route_all.at[me], ts_sem.at[k], tr_sem.at[me], k))
        sent.append(send(gate_all.at[me], gate_all.at[me], gts_sem.at[k], gtr_sem.at[me], k))
    wait(own[2:])
    half = td // 2

    def x_half(s, h):
        return x_all.at[s, pl.ds(h * half, half)]

    def x_send(s, h, k):
        i = len(x_sent)
        x_sent.append(send(x_half(s, h), x_half(s, h), xs_sem.at[i], xr_sem.at[2 * s + h], k))

    def x_wait(s, h):
        arrive(x_half(s, h), xs_sem.at[0], xr_sem.at[2 * s + h])

    x_sent = []
    for h in range(2):
        x_send(me, h, 2)
        x_send(me, 1 - h, 4)
    for h in range(2):
        x_send(me, h, 1)

    for k in range(1, n_src):
        s = peer(k)[1]
        arrive(route_all.at[s], ts_sem.at[k], tr_sem.at[s])
        arrive(gate_all.at[s], gts_sem.at[k], gtr_sem.at[s])

    experts = lax.broadcasted_iota(jnp.int32, (el, td), 0) + me * el
    before = (lax.broadcasted_iota(jnp.int32, (td, td), 0) < lax.broadcasted_iota(jnp.int32, (td, td), 1))
    before = jnp.where(before, 1.0, 0.0).astype(BF)
    place = lax.broadcasted_iota(jnp.int32, (el, ROWS, td), 1).astype(F32)

    def gates_of(s):
        gate = jnp.zeros((el, td), F32)
        for j in range(top):
            gate = jnp.where(route_all[s, j:j + 1, :] == experts, gate_all[s, j:j + 1, :], gate)
        return gate

    def tables(s, _):
        hit = jnp.zeros((el, td), F32)
        for j in range(top):
            hit = jnp.where(route_all[s, j:j + 1, :] == experts, 1.0, hit)
        rank = jnp.where(hit > 0, _dot(hit.astype(BF), before), -1.0)
        sel = jnp.broadcast_to(rank[:, None, :], place.shape) == place
        hot = jnp.where(sel, 1.0, 0.0).reshape(el * ROWS, td)
        onehot[s] = hot.astype(BF)
        onehot_t[s] = hot.T.astype(BF)
        g = jnp.where(sel, jnp.broadcast_to(gates_of(s)[:, None, :], place.shape), 0.0)
        g = g.reshape(el * ROWS, td).T
        for i in range(3):
            part = g.astype(BF)
            gate3_t[s, i * td:(i + 1) * td, :] = part
            g = g - part.astype(F32)
        return 0

    lax.fori_loop(0, n_src, tables, 0)

    def rows_of(s):
        return pl.ds(pl.multiple_of(s * ROWS, ROWS), ROWS)

    def dispatch_x(k):
        s = peer(k)[1]
        xg[:, rows_of(s), :] = _dot(onehot[s], x_all[s]).astype(BF).reshape(el, ROWS, dm)

    dispatch_x(0)
    near_x, near_y, diagonal = peer(2)[1], peer(4)[1], peer(6)[1]
    x_wait(near_x, 0)
    x_send(near_x, 0, 4)
    x_send(near_x, 0, 1)
    x_wait(near_y, 1)
    x_send(near_y, 1, 2)
    x_send(near_y, 1, 1)
    for h in range(2):
        x_wait(peer(1)[1], h)
    dispatch_x(1)
    x_wait(near_x, 1)
    x_send(near_x, 1, 1)
    x_wait(near_y, 0)
    x_send(near_y, 0, 1)
    for k in (2, 4):
        dispatch_x(k)
    for k in (3, 5):
        for h in range(2):
            x_wait(peer(k)[1], h)
        dispatch_x(k)
    for h in range(2):
        x_wait(diagonal, h)
        x_send(diagonal, h, 1)
    for k in (2, 4, 6, 1):
        sent.append(send(dy_all.at[me], dy_all.at[me], ys_sem.at[k], yr_sem.at[me], k))
    dispatch_x(6)
    for h in range(2):
        x_wait(peer(7)[1], h)
    dispatch_x(7)
    sent += x_sent

    def group(p):
        return [p * GROUP + i for i in range(GROUP)]

    groups = el // GROUP

    def forward_hidden(e):
        slot = e % SLOTS
        xe = xg[e]
        ue = _dot(xe, w1[slot]).astype(BF)
        ve = _dot(xe, w3[slot]).astype(BF)
        u[e] = ue
        v[e] = ve
        uf = ue.astype(F32)
        act[e] = (uf * jax.nn.sigmoid(uf) * ve.astype(F32)).astype(BF)

    def forward_out(e):
        o[e] = _dot(act[e], w2[e % SLOTS]).astype(BF)

    def ahead(copies, es):
        for e in es:
            @pl.when(e + SLOTS < el)
            def _():
                start(copies(e + SLOTS))

    def forward(p, _):
        prev, now = group(p - 1), group(p)
        for e in prev:
            wait(down(e))
        for e in now:
            wait(up(e))
        for e in prev:
            forward_out(e)
        for e in now:
            forward_hidden(e)
        ahead(down, prev)
        ahead(up, now)
        return 0

    for e in group(0):
        wait(up(e))
    for e in group(0):
        forward_hidden(e)
    for e in group(0):
        start(up(e + SLOTS))
    lax.fori_loop(1, groups, forward, 0)
    for e in group(groups - 1):
        wait(down(e))
    for e in group(groups - 1):
        forward_out(e)

    def y_part(s):
        z = _dot(gate3_t[s], o[:, rows_of(s), :].reshape(el * ROWS, dm))
        return z[:td] + z[td:2 * td] + z[2 * td:]

    def y_half(j, h):
        return y_own.at[j, pl.ds(h * half, half)]

    def far_send(j, h, i, k):
        sent.append(send(y_half(j, h), y_far.at[i], yf_s.at[i], yf_r.at[i], k))

    def far_add(i, j, h):
        arrive(y_far.at[i], yf_s.at[i], yf_r.at[i])
        y_half(j, h)[...] = y_half(j, h)[...] + y_far[i]

    def far_forward():
        far_add(0, 2, 0)
        far_send(2, 0, 4, 4)
        far_add(1, 1, 1)
        far_send(1, 1, 5, 2)
        far_add(2, 0, 0)
        far_add(3, 0, 1)

    chip = []
    for j in range(4):
        y_send[j] = y_part(peer(2 * j + 1)[1])
        chip.append(send(y_send.at[j], y_chip.at[j], yc_s.at[j], yc_r.at[j], 1))
    for k in (2, 4, 6):
        s = peer(k)[1]
        arrive(dy_all.at[s], ys_sem.at[k], yr_sem.at[s])
        sent.append(send(dy_all.at[s], dy_all.at[s], ys_sem.at[k + 1], yr_sem.at[s], 1))
    for j in range(4):
        y_own[j] = y_part(peer(2 * j)[1])
    for j in (3, 1, 2, 0):
        arrive(y_chip.at[j], yc_s.at[j], yc_r.at[j])
        y_own[j] = y_own[j] + y_chip[j]
        if j == 2:
            far_send(3, 0, 0, 2)
            far_send(3, 1, 1, 4)
            far_send(1, 0, 2, 2)
            far_send(2, 1, 3, 4)

    def dispatch_dy(s):
        gate = gates_of(s)
        dgt = []
        part = el // 4
        for h in range(4):
            es = slice(h * part, (h + 1) * part)
            hot = onehot[s, h * part * ROWS:(h + 1) * part * ROWS, :]
            d = _dot(hot, dy_all[s])
            hot = hot.astype(F32)
            os = o[es, rows_of(s), :].reshape(part * ROWS, dm).astype(F32)
            dg = jnp.sum(d * os, axis=1, keepdims=True)
            dgt.append(jnp.sum((hot * dg).reshape(part, ROWS, td), axis=1))
            g = jnp.broadcast_to(gate[es][:, None, :], (part, ROWS, td)).reshape(part * ROWS, td)
            g = jnp.sum(hot * g, axis=1, keepdims=True)
            q[es, rows_of(s), :] = (g * d).astype(BF).reshape(part, ROWS, dm)
        dgt = jnp.concatenate(dgt, axis=0)
        for j in range(top):
            m = route_all[s, j:j + 1, :] == experts
            dg_send[s, j:j + 1, :] = jnp.sum(jnp.where(m, dgt, 0.0), axis=0, keepdims=True)

    for k in (0, 1, 2, 4, 6, 3, 5, 7):
        s = peer(k)[1]
        if k in (1, 3, 5, 7):
            arrive(dy_all.at[s], ys_sem.at[k], yr_sem.at[s])
        dispatch_dy(s)
        if k:
            sent.append(send(dg_send.at[s], dg_all.at[me], gs_sem.at[k], gr_sem.at[me], k))
        else:
            dg_all[me] = dg_send[s]

    def backward_hidden(e):
        da = _dot(q[e], w2[e % SLOTS], DIM1).astype(BF).astype(F32)
        uf = u[e].astype(F32)
        vf = v[e].astype(F32)
        sg = jax.nn.sigmoid(uf)
        u[e] = (da * vf * sg * (1 + uf * (1 - sg))).astype(BF)
        v[e] = (da * (uf * sg)).astype(BF)

    def backward_out(e):
        slot = e % SLOTS
        o[e] = (_dot(u[e], w1[slot], DIM1) + _dot(v[e], w3[slot], DIM1)).astype(BF)

    def refill(copies, es):
        for e in es:
            @pl.when(e >= SLOTS)
            def _():
                start(copies(e - SLOTS))

    def ready(copies, es):
        for e in es:
            @pl.when(e < el - SLOTS)
            def _():
                wait(copies(e))

    def down_group(p):
        return [el - 1 - (p * GROUP + i) for i in range(GROUP)]

    def backward(p, _):
        prev, now = down_group(p - 1), down_group(p)
        ready(up, prev)
        ready(down, now)
        for e in prev:
            backward_out(e)
        for e in now:
            backward_hidden(e)
        refill(up, prev)
        refill(down, now)
        return 0

    for e in down_group(0):
        backward_hidden(e)
    refill(down, down_group(0))
    lax.fori_loop(1, FORWARD_AT, backward, 0)
    far_forward()
    lax.fori_loop(FORWARD_AT, groups, backward, 0)
    ready(up, down_group(groups - 1))
    for e in down_group(groups - 1):
        backward_out(e)

    for k in range(1, n_src):
        s = peer(k)[1]
        arrive(dg_all.at[s], gs_sem.at[k], gr_sem.at[s])
    for c in chip:
        c.wait_send()

    def dx_part(s):
        return _dot(onehot_t[s], o[:, rows_of(s), :].reshape(el * ROWS, dm))

    for j in range(4):
        y_send[j] = dx_part(peer(2 * j + 1)[1])
        sent.append(send(y_send.at[j], y_chip.at[j], dc_s.at[j], dc_r.at[j], 1))
    for j in range(4):
        d_own[j] = dx_part(peer(2 * j)[1])
    for i, h in ((4, 0), (5, 1)):
        far_add(i, 0, h)
    y_out[...] = y_own[0].astype(BF)
    dg_out[...] = jnp.sum(dg_all[...], axis=0)

    outs = []
    for j, out in ((3, dx3), (1, dx1), (2, dx2), (0, dx0)):
        arrive(y_chip.at[j], dc_s.at[j], dc_r.at[j])
        d_own[j] = d_own[j] + y_chip[j]
        outs.append(pltpu.make_async_copy(d_own.at[j], out, out_sem.at[j]))
        outs[-1].start()

    for c in sent:
        c.wait_send()
    wait(outs)


def _grad_kernel(xg, q, act, du, dv, y, dg, dw1, dw3, dw2, y_out, dg_out):
    for i in range(xg.shape[0]):
        dw1[i] = _dot(xg[i], du[i], DIM0)
        dw3[i] = _dot(xg[i], dv[i], DIM0)
        dw2[i] = _dot(act[i], q[i], DIM0)
    y_out[...] = y[...]
    dg_out[...] = dg[...]


def solution(mesh):
    ep = ('row', 'col', 'core')
    n_src = mesh.shape['row'] * mesh.shape['col'] * mesh.shape['core']
    tspec = P(('dp',) + ep, None)
    wspec = P(ep, None, None)
    gspec = P(('dp',) + ep, None, None)

    def body(x, route_idx, gates, w1, w3, w2, dy):
        td, top = route_idx.shape
        el, dm, fh = w1.shape
        er = n_src * ROWS
        sds = jax.ShapeDtypeStruct
        vmem = pltpu.VMEM
        dma = pltpu.SemaphoreType.DMA
        block = (td, dm)
        small = (n_src, top, td)
        whole = pl.BlockSpec(memory_space=pltpu.VMEM)
        flops = 2 * el * er * dm * fh * 6
        xg, q, act, du, dv, y, dg, dx0, dx1, dx2, dx3 = pl.pallas_call(
            _core_kernel,
            name='moe_core',
            out_shape=[vmem((el, er, dm), BF), vmem((el, er, dm), BF)] + [vmem((el, er, fh), BF)] * 3
            + [vmem(block, BF), vmem((top, td), F32)] + [sds(block, F32)] * 4,
            in_specs=[ANY] * 7,
            out_specs=[whole] * 7 + [ANY] * 4,
            scratch_shapes=[
                vmem((n_src,) + block, BF), vmem((n_src,) + block, BF), vmem(small, jnp.int32), vmem(small, F32),
                vmem((el, er, dm), BF),
                vmem((n_src, el * ROWS, td), BF), vmem((n_src, td, el * ROWS), BF), vmem((n_src, 3 * td, el * ROWS), BF),
                vmem((SLOTS, dm, fh), BF), vmem((SLOTS, dm, fh), BF), vmem((SLOTS, fh, dm), BF),
                vmem((4,) + block, F32), vmem((4,) + block, F32), vmem((4,) + block, F32), vmem((6, td // 2, dm), F32),
                vmem((4,) + block, F32), vmem(small, F32), vmem(small, F32),
                dma((4,)), dma((3, SLOTS)), dma((4,)),
                dma((16,)), dma((16,)), dma((8,)), dma((8,)), dma((8,)), dma((8,)), dma((8,)), dma((8,)),
                dma((4,)), dma((4,)), dma((6,)), dma((6,)), dma((4,)), dma((4,)), dma((8,)), dma((8,)),
            ],
            compiler_params=pltpu.CompilerParams(collective_id=0, has_side_effects=True, vmem_limit_bytes=CORE_VMEM << 20),
            cost_estimate=pl.CostEstimate(flops=flops, bytes_accessed=88 << 20, transcendentals=0),
        )(x, dy, route_idx.T, gates.T, w1, w3, w2)

        def swap(a, k):
            return lax.ppermute(a, ep, [(i, i ^ k) for i in range(n_src)])

        far = [swap(dx3, 6), swap(dx1, 2), swap(dx2, 4)]
        per = 2
        spec = lambda a, b: pl.BlockSpec((per, a, b), lambda i: (i, 0, 0))
        once = lambda a, b: pl.BlockSpec((a, b), lambda i: (0, 0))

        dw1, dw3, dw2, y, dg = pl.pallas_call(
            _grad_kernel,
            name='moe_grad',
            grid=(el // per,),
            out_shape=[sds((el, dm, fh), F32), sds((el, dm, fh), F32), sds((el, fh, dm), F32), sds(block, BF), sds((top, td), F32)],
            in_specs=[spec(er, dm), spec(er, dm), spec(er, fh), spec(er, fh), spec(er, fh), once(td, dm), once(top, td)],
            out_specs=[spec(dm, fh), spec(dm, fh), spec(fh, dm), once(td, dm), once(top, td)],
            compiler_params=pltpu.CompilerParams(vmem_limit_bytes=GRAD_VMEM << 20),
            cost_estimate=pl.CostEstimate(flops=2 * el * er * dm * fh * 3, bytes_accessed=90 << 20, transcendentals=0),
        )(xg, q, act, du, dv, y, dg)
        dx = (dx0 + far[0] + far[1] + far[2]).astype(BF)
        return y, dx, dg.T, dw1, dw3, dw2

    return jax.shard_map(body, mesh=mesh, in_specs=(tspec, tspec, tspec, wspec, wspec, wspec, tspec),
                         out_specs=(tspec, tspec, tspec, gspec, gspec, gspec), check_vma=False)
```

```python
import functools

import jax
import jax.numpy as jnp
from jax import lax
from jax.experimental import pallas as pl
from jax.experimental.pallas import tpu as pltpu
from jax.sharding import PartitionSpec as P

MESH = pl.DeviceIdType.MESH
F32 = jnp.float32
BF = jnp.bfloat16
ROWS = 16
SLOTS = 12
CORE_VMEM = 41
GRAD_VMEM = 14
GROUP = 4
DIM0 = (((0,), (0,)), ((), ()))
DIM1 = (((1,), (1,)), ((), ()))
ANY = pl.BlockSpec(memory_space=pl.ANY)


def _dot(a, b, dims=(((1,), (0,)), ((), ()))):
    return lax.dot_general(a, b, dims, preferred_element_type=F32)


def _core_kernel(x_hbm, dy_hbm, route_hbm, gate_hbm, w1_hbm, w3_hbm, w2_hbm,
                 xg, q, act, u, v, dg_out, y_here, dx_here, to_x, to_y, to_xy,
                 x_all, dy_all, route_all, gate_all, o, onehot, onehot_t, gate3_t,
                 w1, w3, w2, y_send, y_own, y_chip, y_far, dg_send, dg_all,
                 in_sem, w_sem,
                 xs_sem, xr_sem, ys_sem, yr_sem, ts_sem, tr_sem, gts_sem, gtr_sem,
                 yc_s, yc_r, yf_s, yf_r, dc_s, dc_r, gs_sem, gr_sem):
    row, col, core = lax.axis_index('row'), lax.axis_index('col'), lax.axis_index('core')
    el, dm, fh = w1_hbm.shape
    td = x_hbm.shape[0]
    top = route_hbm.shape[0]
    n_src = x_all.shape[0]

    def peer(k):
        r = 1 - row if k & 4 else row
        c = 1 - col if k & 2 else col
        h = 1 - core if k & 1 else core
        return {'row': r, 'col': c, 'core': h}, r * 4 + c * 2 + h

    me = peer(0)[1]

    def start(copies):
        for c in copies:
            c.start()

    def wait(copies):
        for c in copies:
            c.wait()

    own = [pltpu.make_async_copy(a, b.at[me], in_sem.at[i])
           for i, (a, b) in enumerate(((route_hbm, route_all), (gate_hbm, gate_all), (x_hbm, x_all), (dy_hbm, dy_all)))]
    start(own)

    def up(e):
        slot = e % SLOTS
        return [pltpu.make_async_copy(a.at[e], b.at[slot], w_sem.at[j, slot])
                for j, (a, b) in enumerate(((w1_hbm, w1), (w3_hbm, w3)))]

    def down(e):
        return [pltpu.make_async_copy(w2_hbm.at[e], w2.at[e % SLOTS], w_sem.at[2, e % SLOTS])]

    barrier = pltpu.get_barrier_semaphore()
    for k in range(1, n_src):
        pl.semaphore_signal(barrier, inc=1, device_id=peer(k)[0], device_id_type=MESH)
    for e in range(SLOTS):
        start(up(e) + down(e))
    pl.semaphore_wait(barrier, n_src - 1)

    def send(src, dst, s_sem, r_sem, k):
        c = pltpu.make_async_remote_copy(src_ref=src, dst_ref=dst, send_sem=s_sem, recv_sem=r_sem,
                                         device_id=peer(k)[0], device_id_type=MESH)
        c.start()
        return c

    def arrive(dst, s_sem, r_sem):
        pltpu.make_async_remote_copy(src_ref=dst, dst_ref=dst, send_sem=s_sem, recv_sem=r_sem,
                                     device_id=peer(1)[0], device_id_type=MESH).wait_recv()

    sent = []
    wait(own[:2])
    for k in range(1, n_src):
        sent.append(send(route_all.at[me], route_all.at[me], ts_sem.at[k], tr_sem.at[me], k))
        sent.append(send(gate_all.at[me], gate_all.at[me], gts_sem.at[k], gtr_sem.at[me], k))
    wait(own[2:])
    half = td // 2

    def x_half(s, h):
        return x_all.at[s, pl.ds(h * half, half)]

    def x_send(s, h, k):
        i = len(x_sent)
        x_sent.append(send(x_half(s, h), x_half(s, h), xs_sem.at[i], xr_sem.at[2 * s + h], k))

    def x_wait(s, h):
        arrive(x_half(s, h), xs_sem.at[0], xr_sem.at[2 * s + h])

    x_sent = []
    for h in range(2):
        x_send(me, h, 2)
        x_send(me, 1 - h, 4)
    for h in range(2):
        x_send(me, h, 1)

    for k in range(1, n_src):
        s = peer(k)[1]
        arrive(route_all.at[s], ts_sem.at[k], tr_sem.at[s])
        arrive(gate_all.at[s], gts_sem.at[k], gtr_sem.at[s])

    experts = lax.broadcasted_iota(jnp.int32, (el, td), 0) + me * el
    before = (lax.broadcasted_iota(jnp.int32, (td, td), 0) < lax.broadcasted_iota(jnp.int32, (td, td), 1))
    before = jnp.where(before, 1.0, 0.0).astype(BF)
    place = lax.broadcasted_iota(jnp.int32, (el, ROWS, td), 1).astype(F32)

    def gates_of(s):
        gate = jnp.zeros((el, td), F32)
        for j in range(top):
            gate = jnp.where(route_all[s, j:j + 1, :] == experts, gate_all[s, j:j + 1, :], gate)
        return gate

    def tables(s, _):
        hit = jnp.zeros((el, td), F32)
        for j in range(top):
            hit = jnp.where(route_all[s, j:j + 1, :] == experts, 1.0, hit)
        rank = jnp.where(hit > 0, _dot(hit.astype(BF), before), -1.0)
        sel = jnp.broadcast_to(rank[:, None, :], place.shape) == place
        hot = jnp.where(sel, 1.0, 0.0).reshape(el * ROWS, td)
        onehot[s] = hot.astype(BF)
        onehot_t[s] = hot.T.astype(BF)
        g = jnp.where(sel, jnp.broadcast_to(gates_of(s)[:, None, :], place.shape), 0.0)
        g = g.reshape(el * ROWS, td).T
        for i in range(3):
            part = g.astype(BF)
            gate3_t[s, i * td:(i + 1) * td, :] = part
            g = g - part.astype(F32)
        return 0

    lax.fori_loop(0, n_src, tables, 0)

    def rows_of(s):
        return pl.ds(pl.multiple_of(s * ROWS, ROWS), ROWS)

    def dispatch_x(k):
        s = peer(k)[1]
        xg[:, rows_of(s), :] = _dot(onehot[s], x_all[s]).astype(BF).reshape(el, ROWS, dm)

    dispatch_x(0)
    near_x, near_y, diagonal = peer(2)[1], peer(4)[1], peer(6)[1]
    x_wait(near_x, 0)
    x_send(near_x, 0, 4)
    x_send(near_x, 0, 1)
    x_wait(near_y, 1)
    x_send(near_y, 1, 2)
    x_send(near_y, 1, 1)
    for h in range(2):
        x_wait(peer(1)[1], h)
    dispatch_x(1)
    x_wait(near_x, 1)
    x_send(near_x, 1, 1)
    x_wait(near_y, 0)
    x_send(near_y, 0, 1)
    for k in (2, 4):
        dispatch_x(k)
    for k in (3, 5):
        for h in range(2):
            x_wait(peer(k)[1], h)
        dispatch_x(k)
    for h in range(2):
        x_wait(diagonal, h)
        x_send(diagonal, h, 1)
    for k in (2, 4, 6, 1):
        sent.append(send(dy_all.at[me], dy_all.at[me], ys_sem.at[k], yr_sem.at[me], k))
    dispatch_x(6)
    for h in range(2):
        x_wait(peer(7)[1], h)
    dispatch_x(7)
    sent += x_sent

    def group(p):
        return [p * GROUP + i for i in range(GROUP)]

    groups = el // GROUP

    def forward_hidden(e):
        slot = e % SLOTS
        xe = xg[e]
        ue = _dot(xe, w1[slot]).astype(BF)
        ve = _dot(xe, w3[slot]).astype(BF)
        u[e] = ue
        v[e] = ve
        uf = ue.astype(F32)
        act[e] = (uf * jax.nn.sigmoid(uf) * ve.astype(F32)).astype(BF)

    def forward_out(e):
        o[e] = _dot(act[e], w2[e % SLOTS]).astype(BF)

    def ahead(copies, es):
        for e in es:
            @pl.when(e + SLOTS < el)
            def _():
                start(copies(e + SLOTS))

    def forward(p, _):
        prev, now = group(p - 1), group(p)
        for e in prev:
            wait(down(e))
        for e in now:
            wait(up(e))
        for e in prev:
            forward_out(e)
        for e in now:
            forward_hidden(e)
        ahead(down, prev)
        ahead(up, now)
        return 0

    for e in group(0):
        wait(up(e))
    for e in group(0):
        forward_hidden(e)
    for e in group(0):
        start(up(e + SLOTS))
    lax.fori_loop(1, groups, forward, 0)
    for e in group(groups - 1):
        wait(down(e))
    for e in group(groups - 1):
        forward_out(e)

    def y_part(s):
        z = _dot(gate3_t[s], o[:, rows_of(s), :].reshape(el * ROWS, dm))
        return z[:td] + z[td:2 * td] + z[2 * td:]

    def y_half(j, h):
        return y_own.at[j, pl.ds(h * half, half)]

    def far_send(j, h, i, k):
        sent.append(send(y_half(j, h), y_far.at[i], yf_s.at[i], yf_r.at[i], k))

    def far_sum(i, j, h):
        arrive(y_far.at[i], yf_s.at[i], yf_r.at[i])
        return y_half(j, h)[...] + y_far[i]

    chip = []
    for j in range(4):
        y_send[j] = y_part(peer(2 * j + 1)[1])
        chip.append(send(y_send.at[j], y_chip.at[j], yc_s.at[j], yc_r.at[j], 1))
    for k in (2, 4, 6):
        s = peer(k)[1]
        arrive(dy_all.at[s], ys_sem.at[k], yr_sem.at[s])
        sent.append(send(dy_all.at[s], dy_all.at[s], ys_sem.at[k + 1], yr_sem.at[s], 1))
    for j in range(4):
        y_own[j] = y_part(peer(2 * j)[1])
    for j in (3, 1, 2, 0):
        arrive(y_chip.at[j], yc_s.at[j], yc_r.at[j])
        y_own[j] = y_own[j] + y_chip[j]
        if j == 2:
            far_send(3, 0, 0, 2)
            far_send(3, 1, 1, 4)
            far_send(1, 0, 2, 2)
            far_send(2, 1, 3, 4)

    def dispatch_dy(s):
        gate = gates_of(s)
        dgt = []
        part = el // 4
        for h in range(4):
            es = slice(h * part, (h + 1) * part)
            hot = onehot[s, h * part * ROWS:(h + 1) * part * ROWS, :]
            d = _dot(hot, dy_all[s])
            hot = hot.astype(F32)
            os = o[es, rows_of(s), :].reshape(part * ROWS, dm).astype(F32)
            dg = jnp.sum(d * os, axis=1, keepdims=True)
            dgt.append(jnp.sum((hot * dg).reshape(part, ROWS, td), axis=1))
            g = jnp.broadcast_to(gate[es][:, None, :], (part, ROWS, td)).reshape(part * ROWS, td)
            g = jnp.sum(hot * g, axis=1, keepdims=True)
            q[es, rows_of(s), :] = (g * d).astype(BF).reshape(part, ROWS, dm)
        dgt = jnp.concatenate(dgt, axis=0)
        for j in range(top):
            m = route_all[s, j:j + 1, :] == experts
            dg_send[s, j:j + 1, :] = jnp.sum(jnp.where(m, dgt, 0.0), axis=0, keepdims=True)

    for k in (0, 1, 2, 4, 6, 3, 5, 7):
        s = peer(k)[1]
        if k in (1, 3, 5, 7):
            arrive(dy_all.at[s], ys_sem.at[k], yr_sem.at[s])
        dispatch_dy(s)
        if k:
            sent.append(send(dg_send.at[s], dg_all.at[me], gs_sem.at[k], gr_sem.at[me], k))
        else:
            dg_all[me] = dg_send[s]

    def backward_hidden(e):
        da = _dot(q[e], w2[e % SLOTS], DIM1).astype(BF).astype(F32)
        uf = u[e].astype(F32)
        vf = v[e].astype(F32)
        sg = jax.nn.sigmoid(uf)
        u[e] = (da * vf * sg * (1 + uf * (1 - sg))).astype(BF)
        v[e] = (da * (uf * sg)).astype(BF)

    def backward_out(e):
        slot = e % SLOTS
        o[e] = (_dot(u[e], w1[slot], DIM1) + _dot(v[e], w3[slot], DIM1)).astype(BF)

    def refill(copies, es):
        for e in es:
            @pl.when(e >= SLOTS)
            def _():
                start(copies(e - SLOTS))

    def ready(copies, es):
        for e in es:
            @pl.when(e < el - SLOTS)
            def _():
                wait(copies(e))

    def down_group(p):
        return [el - 1 - (p * GROUP + i) for i in range(GROUP)]

    def backward(p, _):
        prev, now = down_group(p - 1), down_group(p)
        ready(up, prev)
        ready(down, now)
        for e in prev:
            backward_out(e)
        for e in now:
            backward_hidden(e)
        refill(up, prev)
        refill(down, now)
        return 0

    for e in down_group(0):
        backward_hidden(e)
    refill(down, down_group(0))
    lax.fori_loop(1, groups, backward, 0)
    ready(up, down_group(groups - 1))
    for e in down_group(groups - 1):
        backward_out(e)

    for k in range(1, n_src):
        s = peer(k)[1]
        arrive(dg_all.at[s], gs_sem.at[k], gr_sem.at[s])
    for c in chip:
        c.wait_send()

    def dx_part(s):
        return _dot(onehot_t[s], o[:, rows_of(s), :].reshape(el * ROWS, dm))

    for j in range(4):
        y_send[j] = dx_part(peer(2 * j + 1)[1])
        sent.append(send(y_send.at[j], y_chip.at[j], dc_s.at[j], dc_r.at[j], 1))
    d_own = (dx_here, to_x.at[pl.ds(0, td)], to_y.at[pl.ds(0, td)], to_xy)
    for j in range(4):
        d_own[j][...] = dx_part(peer(2 * j)[1])

    to_y[pl.ds(td, half), :] = far_sum(0, 2, 0)
    to_x[pl.ds(td, half), :] = far_sum(1, 1, 1)
    y_here[pl.ds(0, half), :] = far_sum(2, 0, 0)
    y_here[pl.ds(half, half), :] = far_sum(3, 0, 1)
    dg_out[...] = jnp.sum(dg_all[...], axis=0)

    for j in range(4):
        arrive(y_chip.at[j], dc_s.at[j], dc_r.at[j])
        d_own[j][...] = d_own[j][...] + y_chip[j]

    for c in sent:
        c.wait_send()


def _grad_kernel(xg, q, act, du, dv, dg, dw1, dw3, dw2, dg_out):
    for i in range(xg.shape[0]):
        dw1[i] = _dot(xg[i], du[i], DIM0)
        dw3[i] = _dot(xg[i], dv[i], DIM0)
        dw2[i] = _dot(act[i], q[i], DIM0)
    dg_out[...] = dg[...]


def solution(mesh):
    ep = ('row', 'col', 'core')
    n_src = mesh.shape['row'] * mesh.shape['col'] * mesh.shape['core']
    tspec = P(('dp',) + ep, None)
    wspec = P(ep, None, None)
    gspec = P(('dp',) + ep, None, None)

    def body(x, route_idx, gates, w1, w3, w2, dy):
        td, top = route_idx.shape
        el, dm, fh = w1.shape
        er = n_src * ROWS
        sds = jax.ShapeDtypeStruct
        vmem = pltpu.VMEM
        dma = pltpu.SemaphoreType.DMA
        block = (td, dm)
        small = (n_src, top, td)
        whole = pl.BlockSpec(memory_space=pltpu.VMEM)
        flops = 2 * el * er * dm * fh * 6
        xg, q, act, du, dv, dg, y_here, dx_here, to_x, to_y, to_xy = pl.pallas_call(
            _core_kernel,
            name='moe_core',
            out_shape=[vmem((el, er, dm), BF), vmem((el, er, dm), BF)] + [vmem((el, er, fh), BF)] * 3
            + [vmem((top, td), F32), vmem(block, F32), vmem(block, F32)]
            + [vmem((td + td // 2, dm), F32)] * 2 + [vmem(block, F32)],
            in_specs=[ANY] * 7,
            out_specs=[whole] * 11,
            scratch_shapes=[
                vmem((n_src,) + block, BF), vmem((n_src,) + block, BF), vmem(small, jnp.int32), vmem(small, F32),
                vmem((el, er, dm), BF),
                vmem((n_src, el * ROWS, td), BF), vmem((n_src, td, el * ROWS), BF), vmem((n_src, 3 * td, el * ROWS), BF),
                vmem((SLOTS, dm, fh), BF), vmem((SLOTS, dm, fh), BF), vmem((SLOTS, fh, dm), BF),
                vmem((4,) + block, F32), vmem((4,) + block, F32), vmem((4,) + block, F32), vmem((4, td // 2, dm), F32),
                vmem(small, F32), vmem(small, F32),
                dma((4,)), dma((3, SLOTS)),
                dma((16,)), dma((16,)), dma((8,)), dma((8,)), dma((8,)), dma((8,)), dma((8,)), dma((8,)),
                dma((4,)), dma((4,)), dma((4,)), dma((4,)), dma((4,)), dma((4,)), dma((8,)), dma((8,)),
            ],
            compiler_params=pltpu.CompilerParams(collective_id=0, has_side_effects=True, vmem_limit_bytes=CORE_VMEM << 20),
            cost_estimate=pl.CostEstimate(flops=flops, bytes_accessed=88 << 20, transcendentals=0),
        )(x, dy, route_idx.T, gates.T, w1, w3, w2)

        def swap(a, k):
            return lax.ppermute(a, ep, [(i, i ^ k) for i in range(n_src)])

        from_xy, from_x, from_y = swap(to_xy, 6), swap(to_x, 2), swap(to_y, 4)
        per = 2
        spec = lambda a, b: pl.BlockSpec((per, a, b), lambda i: (i, 0, 0))
        once = lambda a, b: pl.BlockSpec((a, b), lambda i: (0, 0))

        dw1, dw3, dw2, dg = pl.pallas_call(
            _grad_kernel,
            name='moe_grad',
            grid=(el // per,),
            out_shape=[sds((el, dm, fh), F32), sds((el, dm, fh), F32), sds((el, fh, dm), F32), sds((top, td), F32)],
            in_specs=[spec(er, dm), spec(er, dm), spec(er, fh), spec(er, fh), spec(er, fh), once(top, td)],
            out_specs=[spec(dm, fh), spec(dm, fh), spec(fh, dm), once(top, td)],
            compiler_params=pltpu.CompilerParams(vmem_limit_bytes=GRAD_VMEM << 20),
            cost_estimate=pl.CostEstimate(flops=2 * el * er * dm * fh * 3, bytes_accessed=90 << 20, transcendentals=0),
        )(xg, q, act, du, dv, dg)
        dx = (dx_here + from_x[:td] + from_y[:td] + from_xy).astype(BF)
        y = (y_here + jnp.concatenate([from_y[td:], from_x[td:]])).astype(BF)
        return y, dx, dg.T, dw1, dw3, dw2

    return jax.shard_map(body, mesh=mesh, in_specs=(tspec, tspec, tspec, wspec, wspec, wspec, tspec),
                         out_specs=(tspec, tspec, tspec, gspec, gspec, gspec), check_vma=False)
```

```python
import functools

import jax
import jax.numpy as jnp
from jax import lax
from jax.experimental import pallas as pl
from jax.experimental.pallas import tpu as pltpu
from jax.sharding import PartitionSpec as P

MESH = pl.DeviceIdType.MESH
F32 = jnp.float32
BF = jnp.bfloat16
ROWS = 16
SLOTS = 12
CORE_VMEM = 41
GRAD_VMEM = 14
GROUP = 4
PARTS = 4
DIM0 = (((0,), (0,)), ((), ()))
DIM1 = (((1,), (1,)), ((), ()))
ANY = pl.BlockSpec(memory_space=pl.ANY)


def _dot(a, b, dims=(((1,), (0,)), ((), ()))):
    return lax.dot_general(a, b, dims, preferred_element_type=F32)


def _core_kernel(x_hbm, dy_hbm, route_hbm, gate_hbm, w1_hbm, w3_hbm, w2_hbm,
                 xg, q, act, u, v, dg_out, y_here, dx_here, to_x, to_y, to_xy,
                 x_all, dy_all, route_all, gate_all, o, onehot, onehot_t, gate3_t,
                 w1, w3, w2, y_send, y_own, y_chip, y_far, dg_send, dg_all,
                 in_sem, w_sem,
                 xs_sem, xr_sem, ys_sem, yr_sem, ts_sem, tr_sem, gts_sem, gtr_sem,
                 yc_s, yc_r, yf_s, yf_r, dc_s, dc_r, gs_sem, gr_sem):
    row, col, core = lax.axis_index('row'), lax.axis_index('col'), lax.axis_index('core')
    el, dm, fh = w1_hbm.shape
    td = x_hbm.shape[0]
    top = route_hbm.shape[0]
    n_src = x_all.shape[0]

    def peer(k):
        r = 1 - row if k & 4 else row
        c = 1 - col if k & 2 else col
        h = 1 - core if k & 1 else core
        return {'row': r, 'col': c, 'core': h}, r * 4 + c * 2 + h

    me = peer(0)[1]

    def start(copies):
        for c in copies:
            c.start()

    def wait(copies):
        for c in copies:
            c.wait()

    own = [pltpu.make_async_copy(a, b.at[me], in_sem.at[i])
           for i, (a, b) in enumerate(((route_hbm, route_all), (gate_hbm, gate_all), (x_hbm, x_all), (dy_hbm, dy_all)))]
    start(own)

    def up(e):
        slot = e % SLOTS
        return [pltpu.make_async_copy(a.at[e], b.at[slot], w_sem.at[j, slot])
                for j, (a, b) in enumerate(((w1_hbm, w1), (w3_hbm, w3)))]

    def down(e):
        return [pltpu.make_async_copy(w2_hbm.at[e], w2.at[e % SLOTS], w_sem.at[2, e % SLOTS])]

    barrier = pltpu.get_barrier_semaphore()
    for k in range(1, n_src):
        pl.semaphore_signal(barrier, inc=1, device_id=peer(k)[0], device_id_type=MESH)
    for e in range(SLOTS):
        start(up(e) + down(e))
    pl.semaphore_wait(barrier, n_src - 1)

    def send(src, dst, s_sem, r_sem, k):
        c = pltpu.make_async_remote_copy(src_ref=src, dst_ref=dst, send_sem=s_sem, recv_sem=r_sem,
                                         device_id=peer(k)[0], device_id_type=MESH)
        c.start()
        return c

    def arrive(dst, s_sem, r_sem):
        pltpu.make_async_remote_copy(src_ref=dst, dst_ref=dst, send_sem=s_sem, recv_sem=r_sem,
                                     device_id=peer(1)[0], device_id_type=MESH).wait_recv()

    sent = []
    wait(own[:2])
    for k in range(1, n_src):
        sent.append(send(route_all.at[me], route_all.at[me], ts_sem.at[k], tr_sem.at[me], k))
        sent.append(send(gate_all.at[me], gate_all.at[me], gts_sem.at[k], gtr_sem.at[me], k))
    wait(own[2:])
    half = td // 2

    def x_half(s, h):
        return x_all.at[s, pl.ds(h * half, half)]

    def x_send(s, h, k):
        i = len(x_sent)
        x_sent.append(send(x_half(s, h), x_half(s, h), xs_sem.at[i], xr_sem.at[2 * s + h], k))

    def x_wait(s, h):
        arrive(x_half(s, h), xs_sem.at[0], xr_sem.at[2 * s + h])

    x_sent = []
    for h in range(2):
        x_send(me, h, 2)
        x_send(me, 1 - h, 4)
    for h in range(2):
        x_send(me, h, 1)

    for k in range(1, n_src):
        s = peer(k)[1]
        arrive(route_all.at[s], ts_sem.at[k], tr_sem.at[s])
        arrive(gate_all.at[s], gts_sem.at[k], gtr_sem.at[s])

    experts = lax.broadcasted_iota(jnp.int32, (el, td), 0) + me * el
    before = (lax.broadcasted_iota(jnp.int32, (td, td), 0) < lax.broadcasted_iota(jnp.int32, (td, td), 1))
    before = jnp.where(before, 1.0, 0.0).astype(BF)
    place = lax.broadcasted_iota(jnp.int32, (el, ROWS, td), 1).astype(F32)

    def gates_of(s):
        gate = jnp.zeros((el, td), F32)
        for j in range(top):
            gate = jnp.where(route_all[s, j:j + 1, :] == experts, gate_all[s, j:j + 1, :], gate)
        return gate

    def tables(s, _):
        hit = jnp.zeros((el, td), F32)
        for j in range(top):
            hit = jnp.where(route_all[s, j:j + 1, :] == experts, 1.0, hit)
        rank = jnp.where(hit > 0, _dot(hit.astype(BF), before), -1.0)
        sel = jnp.broadcast_to(rank[:, None, :], place.shape) == place
        hot = jnp.where(sel, 1.0, 0.0).reshape(el * ROWS, td)
        onehot[s] = hot.astype(BF)
        onehot_t[s] = hot.T.astype(BF)
        g = jnp.where(sel, jnp.broadcast_to(gates_of(s)[:, None, :], place.shape), 0.0)
        g = g.reshape(el * ROWS, td).T
        for i in range(3):
            part = g.astype(BF)
            gate3_t[s, i * td:(i + 1) * td, :] = part
            g = g - part.astype(F32)
        return 0

    lax.fori_loop(0, n_src, tables, 0)

    def rows_of(s):
        return pl.ds(pl.multiple_of(s * ROWS, ROWS), ROWS)

    def dispatch_x(k):
        s = peer(k)[1]
        xg[:, rows_of(s), :] = _dot(onehot[s], x_all[s]).astype(BF).reshape(el, ROWS, dm)

    near_x, near_y, diagonal = peer(2)[1], peer(4)[1], peer(6)[1]
    x_wait(near_x, 0)
    x_send(near_x, 0, 4)
    x_send(near_x, 0, 1)
    x_wait(near_y, 1)
    x_send(near_y, 1, 2)
    x_send(near_y, 1, 1)
    dispatch_x(0)
    for h in range(2):
        x_wait(peer(1)[1], h)
    dispatch_x(1)
    x_wait(near_x, 1)
    x_send(near_x, 1, 1)
    x_wait(near_y, 0)
    x_send(near_y, 0, 1)
    for k in (2, 4):
        dispatch_x(k)
    for k in (3, 5):
        for h in range(2):
            x_wait(peer(k)[1], h)
        dispatch_x(k)
    for h in range(2):
        x_wait(diagonal, h)
        x_send(diagonal, h, 1)
    for k in (2, 4, 6, 1):
        sent.append(send(dy_all.at[me], dy_all.at[me], ys_sem.at[k], yr_sem.at[me], k))
    dispatch_x(6)
    for h in range(2):
        x_wait(peer(7)[1], h)
    dispatch_x(7)
    sent += x_sent

    def group(p):
        return [p * GROUP + i for i in range(GROUP)]

    groups = el // GROUP

    def forward_hidden(e):
        slot = e % SLOTS
        xe = xg[e]
        ue = _dot(xe, w1[slot]).astype(BF)
        ve = _dot(xe, w3[slot]).astype(BF)
        u[e] = ue
        v[e] = ve
        uf = ue.astype(F32)
        act[e] = (uf * jax.nn.sigmoid(uf) * ve.astype(F32)).astype(BF)

    def forward_out(e):
        o[e] = _dot(act[e], w2[e % SLOTS]).astype(BF)

    def ahead(copies, es):
        for e in es:
            @pl.when(e + SLOTS < el)
            def _():
                start(copies(e + SLOTS))

    def forward(p, _):
        prev, now = group(p - 1), group(p)
        for e in prev:
            wait(down(e))
        for e in now:
            wait(up(e))
        for e in prev:
            forward_out(e)
        for e in now:
            forward_hidden(e)
        ahead(down, prev)
        ahead(up, now)
        return 0

    for e in group(0):
        wait(up(e))
    for e in group(0):
        forward_hidden(e)
    for e in group(0):
        start(up(e + SLOTS))
    lax.fori_loop(1, groups, forward, 0)
    for e in group(groups - 1):
        wait(down(e))
    for e in group(groups - 1):
        forward_out(e)

    def y_part(s, out):
        def columns(c):
            n = min(256, dm - c)
            z = _dot(gate3_t[s], o[:, rows_of(s), pl.ds(c, n)].reshape(el * ROWS, n))
            out[:, pl.ds(c, n)] = z[:td] + z[td:2 * td] + z[2 * td:]
        return [functools.partial(columns, c) for c in range(0, dm, 256)]

    def y_half(j, h):
        return y_own.at[j, pl.ds(h * half, half)]

    def far_send(j, h, i, k):
        sent.append(send(y_half(j, h), y_far.at[i], yf_s.at[i], yf_r.at[i], k))

    def far_sum(i, j, h):
        arrive(y_far.at[i], yf_s.at[i], yf_r.at[i])
        return y_half(j, h)[...] + y_far[i]

    def dispatch_dy(s):
        gate = gates_of(s)
        dgt = []
        part = el // PARTS

        def rows(h):
            es = slice(h * part, (h + 1) * part)
            hot = onehot[s, h * part * ROWS:(h + 1) * part * ROWS, :]
            d = _dot(hot, dy_all[s])
            hot = hot.astype(F32)
            os = o[es, rows_of(s), :].reshape(part * ROWS, dm).astype(F32)
            dg = jnp.sum(d * os, axis=1, keepdims=True)
            dgt.append(jnp.sum((hot * dg).reshape(part, ROWS, td), axis=1))
            g = jnp.broadcast_to(gate[es][:, None, :], (part, ROWS, td)).reshape(part * ROWS, td)
            g = jnp.sum(hot * g, axis=1, keepdims=True)
            q[es, rows_of(s), :] = (g * d).astype(BF).reshape(part, ROWS, dm)

        def finish():
            total = jnp.concatenate(dgt, axis=0)
            for j in range(top):
                m = route_all[s, j:j + 1, :] == experts
                dg_send[s, j:j + 1, :] = jnp.sum(jnp.where(m, total, 0.0), axis=0, keepdims=True)

        return [functools.partial(rows, h) for h in range(PARTS)] + [finish]

    def together(y_steps, d_steps):
        each = -(-len(d_steps) // len(y_steps))
        for i, step in enumerate(y_steps):
            step()
            for d_step in d_steps[i * each:(i + 1) * each]:
                d_step()

    chip = []
    for i, k in enumerate((0, 1, 2, 4, 6, 3, 5, 7)):
        j = i % 4
        if i == 1:
            arrive(dy_all.at[peer(1)[1]], ys_sem.at[1], yr_sem.at[peer(1)[1]])
        if i == 2:
            for n in (2, 4, 6):
                s = peer(n)[1]
                arrive(dy_all.at[s], ys_sem.at[n], yr_sem.at[s])
                sent.append(send(dy_all.at[s], dy_all.at[s], ys_sem.at[n + 1], yr_sem.at[s], 1))
        if i == 5:
            for n in (3, 5, 7):
                s = peer(n)[1]
                arrive(dy_all.at[s], ys_sem.at[n], yr_sem.at[s])
        to_chip = i < 4
        together(y_part(peer(2 * j + 1 if to_chip else 2 * j)[1], (y_send if to_chip else y_own).at[j]), dispatch_dy(peer(k)[1]))
        if to_chip:
            chip.append(send(y_send.at[j], y_chip.at[j], yc_s.at[j], yc_r.at[j], 1))
    for j in (3, 1, 2, 0):
        arrive(y_chip.at[j], yc_s.at[j], yc_r.at[j])
        y_own[j] = y_own[j] + y_chip[j]
        if j == 2:
            far_send(3, 0, 0, 2)
            far_send(3, 1, 1, 4)
            far_send(1, 0, 2, 2)
            far_send(2, 1, 3, 4)
    for k in range(n_src):
        s = peer(k)[1]
        if k:
            sent.append(send(dg_send.at[s], dg_all.at[me], gs_sem.at[k], gr_sem.at[me], k))
        else:
            dg_all[me] = dg_send[s]

    def backward_hidden(e):
        da = _dot(q[e], w2[e % SLOTS], DIM1).astype(BF).astype(F32)
        uf = u[e].astype(F32)
        vf = v[e].astype(F32)
        sg = jax.nn.sigmoid(uf)
        return (da * vf * sg * (1 + uf * (1 - sg))).astype(BF), (da * (uf * sg)).astype(BF)

    def backward_hiddens(es):
        for e, (du, dv) in [(e, backward_hidden(e)) for e in es]:
            u[e] = du
            v[e] = dv

    def backward_out(e):
        slot = e % SLOTS
        o[e] = (_dot(u[e], w1[slot], DIM1) + _dot(v[e], w3[slot], DIM1)).astype(BF)

    def refill(copies, es):
        for e in es:
            @pl.when(e >= SLOTS)
            def _():
                start(copies(e - SLOTS))

    def ready(copies, es):
        for e in es:
            @pl.when(e < el - SLOTS)
            def _():
                wait(copies(e))

    def down_group(p):
        return [el - 1 - (p * GROUP + i) for i in range(GROUP)]

    def backward(p, _):
        prev, now = down_group(p - 1), down_group(p)
        ready(up, prev)
        ready(down, now)
        for e in prev:
            backward_out(e)
        backward_hiddens(now)
        refill(up, prev)
        refill(down, now)
        return 0

    backward_hiddens(down_group(0))
    refill(down, down_group(0))
    lax.fori_loop(1, groups, backward, 0)
    ready(up, down_group(groups - 1))
    for e in down_group(groups - 1):
        backward_out(e)

    for k in range(1, n_src):
        s = peer(k)[1]
        arrive(dg_all.at[s], gs_sem.at[k], gr_sem.at[s])
    for c in chip:
        c.wait_send()

    def dx_part(s):
        return _dot(onehot_t[s], o[:, rows_of(s), :].reshape(el * ROWS, dm))

    for j in range(4):
        y_send[j] = dx_part(peer(2 * j + 1)[1])
        sent.append(send(y_send.at[j], y_chip.at[j], dc_s.at[j], dc_r.at[j], 1))
    d_own = (dx_here, to_x.at[pl.ds(0, td)], to_y.at[pl.ds(0, td)], to_xy)
    for j in range(4):
        d_own[j][...] = dx_part(peer(2 * j)[1])

    to_y[pl.ds(td, half), :] = far_sum(0, 2, 0)
    to_x[pl.ds(td, half), :] = far_sum(1, 1, 1)
    y_here[pl.ds(0, half), :] = far_sum(2, 0, 0)
    y_here[pl.ds(half, half), :] = far_sum(3, 0, 1)
    dg_out[...] = jnp.sum(dg_all[...], axis=0)

    for j in range(4):
        arrive(y_chip.at[j], dc_s.at[j], dc_r.at[j])
        d_own[j][...] = d_own[j][...] + y_chip[j]

    for c in sent:
        c.wait_send()


def _grad_kernel(xg, q, act, du, dv, dg, dw1, dw3, dw2, dg_out):
    for i in range(xg.shape[0]):
        dw1[i] = _dot(xg[i], du[i], DIM0)
        dw3[i] = _dot(xg[i], dv[i], DIM0)
        dw2[i] = _dot(act[i], q[i], DIM0)
    dg_out[...] = dg[...]


def solution(mesh):
    ep = ('row', 'col', 'core')
    n_src = mesh.shape['row'] * mesh.shape['col'] * mesh.shape['core']
    tspec = P(('dp',) + ep, None)
    wspec = P(ep, None, None)
    gspec = P(('dp',) + ep, None, None)

    def body(x, route_idx, gates, w1, w3, w2, dy):
        td, top = route_idx.shape
        el, dm, fh = w1.shape
        er = n_src * ROWS
        sds = jax.ShapeDtypeStruct
        vmem = pltpu.VMEM
        dma = pltpu.SemaphoreType.DMA
        block = (td, dm)
        small = (n_src, top, td)
        whole = pl.BlockSpec(memory_space=pltpu.VMEM)
        flops = 2 * el * er * dm * fh * 6
        xg, q, act, du, dv, dg, y_here, dx_here, to_x, to_y, to_xy = pl.pallas_call(
            _core_kernel,
            name='moe_core',
            out_shape=[vmem((el, er, dm), BF), vmem((el, er, dm), BF)] + [vmem((el, er, fh), BF)] * 3
            + [vmem((top, td), F32), vmem(block, F32), vmem(block, F32)]
            + [vmem((td + td // 2, dm), F32)] * 2 + [vmem(block, F32)],
            in_specs=[ANY] * 7,
            out_specs=[whole] * 11,
            scratch_shapes=[
                vmem((n_src,) + block, BF), vmem((n_src,) + block, BF), vmem(small, jnp.int32), vmem(small, F32),
                vmem((el, er, dm), BF),
                vmem((n_src, el * ROWS, td), BF), vmem((n_src, td, el * ROWS), BF), vmem((n_src, 3 * td, el * ROWS), BF),
                vmem((SLOTS, dm, fh), BF), vmem((SLOTS, dm, fh), BF), vmem((SLOTS, fh, dm), BF),
                vmem((4,) + block, F32), vmem((4,) + block, F32), vmem((4,) + block, F32), vmem((4, td // 2, dm), F32),
                vmem(small, F32), vmem(small, F32),
                dma((4,)), dma((3, SLOTS)),
                dma((16,)), dma((16,)), dma((8,)), dma((8,)), dma((8,)), dma((8,)), dma((8,)), dma((8,)),
                dma((4,)), dma((4,)), dma((4,)), dma((4,)), dma((4,)), dma((4,)), dma((8,)), dma((8,)),
            ],
            compiler_params=pltpu.CompilerParams(collective_id=0, has_side_effects=True, vmem_limit_bytes=CORE_VMEM << 20),
            cost_estimate=pl.CostEstimate(flops=flops, bytes_accessed=88 << 20, transcendentals=0),
        )(x, dy, route_idx.T, gates.T, w1, w3, w2)

        def swap(a, k):
            return lax.ppermute(a, ep, [(i, i ^ k) for i in range(n_src)])

        from_xy, from_x, from_y = swap(to_xy, 6), swap(to_x, 2), swap(to_y, 4)
        per = 2
        spec = lambda a, b: pl.BlockSpec((per, a, b), lambda i: (i, 0, 0))
        once = lambda a, b: pl.BlockSpec((a, b), lambda i: (0, 0))

        dw1, dw3, dw2, dg = pl.pallas_call(
            _grad_kernel,
            name='moe_grad',
            grid=(el // per,),
            out_shape=[sds((el, dm, fh), F32), sds((el, dm, fh), F32), sds((el, fh, dm), F32), sds((top, td), F32)],
            in_specs=[spec(er, dm), spec(er, dm), spec(er, fh), spec(er, fh), spec(er, fh), once(top, td)],
            out_specs=[spec(dm, fh), spec(dm, fh), spec(fh, dm), once(top, td)],
            compiler_params=pltpu.CompilerParams(vmem_limit_bytes=GRAD_VMEM << 20),
            cost_estimate=pl.CostEstimate(flops=2 * el * er * dm * fh * 3, bytes_accessed=90 << 20, transcendentals=0),
        )(xg, q, act, du, dv, dg)
        dx = (dx_here + from_x[:td] + from_y[:td] + from_xy).astype(BF)
        y = (y_here + jnp.concatenate([from_y[td:], from_x[td:]])).astype(BF)
        return y, dx, dg.T, dw1, dw3, dw2

    return jax.shard_map(body, mesh=mesh, in_specs=(tspec, tspec, tspec, wspec, wspec, wspec, tspec),
                         out_specs=(tspec, tspec, tspec, gspec, gspec, gspec), check_vma=False)
```

```python
import functools

import jax
import jax.numpy as jnp
from jax import lax
from jax.experimental import pallas as pl
from jax.experimental.pallas import tpu as pltpu
from jax.sharding import PartitionSpec as P

MESH = pl.DeviceIdType.MESH
F32 = jnp.float32
BF = jnp.bfloat16
ROWS = 16
SLOTS = 12
CORE_VMEM = 41
GRAD_VMEM = 14
FINISH_VMEM = 6
GROUP = 4
PARTS = 4
DIM0 = (((0,), (0,)), ((), ()))
DIM1 = (((1,), (1,)), ((), ()))
ANY = pl.BlockSpec(memory_space=pl.ANY)


def _dot(a, b, dims=(((1,), (0,)), ((), ()))):
    return lax.dot_general(a, b, dims, preferred_element_type=F32)


def _core_kernel(x_hbm, dy_hbm, route_hbm, gate_hbm, w1_hbm, w3_hbm, w2_hbm,
                 xg, q, act, u, v, dg_out, y_here, dx_here, to_x, to_y, to_xy,
                 x_all, dy_all, route_all, gate_all, o, onehot, onehot_t, gate3_t,
                 w1, w3, w2, y_send, y_own, y_chip, y_far, dg_send, dg_all,
                 in_sem, w_sem, e_sem,
                 xs_sem, xr_sem, ys_sem, yr_sem, ts_sem, tr_sem, gts_sem, gtr_sem,
                 yc_s, yc_r, yf_s, yf_r, dc_s, dc_r, gs_sem, gr_sem):
    row, col, core = lax.axis_index('row'), lax.axis_index('col'), lax.axis_index('core')
    el, dm, fh = w1_hbm.shape
    late = el - el // w2_hbm.shape[1]
    td = x_hbm.shape[0]
    top = route_hbm.shape[0]
    n_src = x_all.shape[0]

    def peer(k):
        r = 1 - row if k & 4 else row
        c = 1 - col if k & 2 else col
        h = 1 - core if k & 1 else core
        return {'row': r, 'col': c, 'core': h}, r * 4 + c * 2 + h

    me = peer(0)[1]

    def start(copies):
        for c in copies:
            c.start()

    def wait(copies):
        for c in copies:
            c.wait()

    own = [pltpu.make_async_copy(a, b.at[me], in_sem.at[i])
           for i, (a, b) in enumerate(((route_hbm, route_all), (gate_hbm, gate_all), (x_hbm, x_all), (dy_hbm, dy_all)))]
    start(own)

    def up(e):
        slot = e % SLOTS
        return [pltpu.make_async_copy(a.at[e], b.at[slot], w_sem.at[j, slot])
                for j, (a, b) in enumerate(((w1_hbm, w1), (w3_hbm, w3)))]

    def down(e):
        return [pltpu.make_async_copy(w2_hbm.at[e], w2.at[e % SLOTS], w_sem.at[2, e % SLOTS])]

    def down_early(e):
        n = w2_hbm.shape[1]
        return [pltpu.make_async_copy(w2_hbm.at[e], q.at[pl.ds((e - late) * n, n)], e_sem.at[e - late])]

    barrier = pltpu.get_barrier_semaphore()
    for k in range(1, n_src):
        pl.semaphore_signal(barrier, inc=1, device_id=peer(k)[0], device_id_type=MESH)
    for e in range(SLOTS):
        start(up(e) + down(e))
    for e in range(late, el):
        start(down_early(e))
    pl.semaphore_wait(barrier, n_src - 1)

    def send(src, dst, s_sem, r_sem, k):
        c = pltpu.make_async_remote_copy(src_ref=src, dst_ref=dst, send_sem=s_sem, recv_sem=r_sem,
                                         device_id=peer(k)[0], device_id_type=MESH)
        c.start()
        return c

    def arrive(dst, s_sem, r_sem):
        pltpu.make_async_remote_copy(src_ref=dst, dst_ref=dst, send_sem=s_sem, recv_sem=r_sem,
                                     device_id=peer(1)[0], device_id_type=MESH).wait_recv()

    sent = []
    wait(own[:2])
    for k in range(1, n_src):
        sent.append(send(route_all.at[me], route_all.at[me], ts_sem.at[k], tr_sem.at[me], k))
        sent.append(send(gate_all.at[me], gate_all.at[me], gts_sem.at[k], gtr_sem.at[me], k))
    wait(own[2:])
    half = td // 2

    def x_half(s, h):
        return x_all.at[s, pl.ds(h * half, half)]

    def x_send(s, h, k):
        i = len(x_sent)
        x_sent.append(send(x_half(s, h), x_half(s, h), xs_sem.at[i], xr_sem.at[2 * s + h], k))

    def x_wait(s, h):
        arrive(x_half(s, h), xs_sem.at[0], xr_sem.at[2 * s + h])

    x_sent = []
    for h in range(2):
        x_send(me, h, 2)
        x_send(me, 1 - h, 4)
    for h in range(2):
        x_send(me, h, 1)

    for k in range(1, n_src):
        s = peer(k)[1]
        arrive(route_all.at[s], ts_sem.at[k], tr_sem.at[s])
        arrive(gate_all.at[s], gts_sem.at[k], gtr_sem.at[s])

    experts = lax.broadcasted_iota(jnp.int32, (el, td), 0) + me * el
    before = (lax.broadcasted_iota(jnp.int32, (td, td), 0) < lax.broadcasted_iota(jnp.int32, (td, td), 1))
    before = jnp.where(before, 1.0, 0.0).astype(BF)
    place = lax.broadcasted_iota(jnp.int32, (el, ROWS, td), 1).astype(F32)

    def gates_of(s):
        gate = jnp.zeros((el, td), F32)
        for j in range(top):
            gate = jnp.where(route_all[s, j:j + 1, :] == experts, gate_all[s, j:j + 1, :], gate)
        return gate

    def tables(s, _):
        hit = jnp.zeros((el, td), F32)
        for j in range(top):
            hit = jnp.where(route_all[s, j:j + 1, :] == experts, 1.0, hit)
        rank = jnp.where(hit > 0, _dot(hit.astype(BF), before), -1.0)
        sel = jnp.broadcast_to(rank[:, None, :], place.shape) == place
        hot = jnp.where(sel, 1.0, 0.0).reshape(el * ROWS, td)
        onehot[s] = hot.astype(BF)
        onehot_t[s] = hot.T.astype(BF)
        g = jnp.where(sel, jnp.broadcast_to(gates_of(s)[:, None, :], place.shape), 0.0)
        g = g.reshape(el * ROWS, td).T
        for i in range(3):
            part = g.astype(BF)
            gate3_t[s, i * td:(i + 1) * td, :] = part
            g = g - part.astype(F32)
        return 0

    lax.fori_loop(0, n_src, tables, 0)

    def rows_of(s):
        return pl.ds(pl.multiple_of(s * ROWS, ROWS), ROWS)

    def dispatch_x(k):
        s = peer(k)[1]
        xg[:, rows_of(s), :] = _dot(onehot[s], x_all[s]).astype(BF).reshape(el, ROWS, dm)

    near_x, near_y, diagonal = peer(2)[1], peer(4)[1], peer(6)[1]
    x_wait(near_x, 0)
    x_send(near_x, 0, 4)
    x_send(near_x, 0, 1)
    x_wait(near_y, 1)
    x_send(near_y, 1, 2)
    x_send(near_y, 1, 1)
    dispatch_x(0)
    for h in range(2):
        x_wait(peer(1)[1], h)
    dispatch_x(1)
    x_wait(near_x, 1)
    x_send(near_x, 1, 1)
    x_wait(near_y, 0)
    x_send(near_y, 0, 1)
    for k in (2, 4):
        dispatch_x(k)
    for k in (3, 5):
        for h in range(2):
            x_wait(peer(k)[1], h)
        dispatch_x(k)
    for h in range(2):
        x_wait(diagonal, h)
        x_send(diagonal, h, 1)
    for k in (2, 4, 6, 1):
        sent.append(send(dy_all.at[me], dy_all.at[me], ys_sem.at[k], yr_sem.at[me], k))
    dispatch_x(6)
    for h in range(2):
        x_wait(peer(7)[1], h)
    dispatch_x(7)
    sent += x_sent

    def group(p):
        return [p * GROUP + i for i in range(GROUP)]

    groups = el // GROUP

    def forward_hidden(e):
        slot = e % SLOTS
        xe = xg[e]
        ue = _dot(xe, w1[slot]).astype(BF)
        ve = _dot(xe, w3[slot]).astype(BF)
        u[e] = ue
        v[e] = ve
        uf = ue.astype(F32)
        act[e] = (uf * jax.nn.sigmoid(uf) * ve.astype(F32)).astype(BF)

    def forward_out(e, early):
        n = w2_hbm.shape[1]
        w = q[pl.ds((e - late) * n, n)] if early else w2[e % SLOTS]
        o[e] = _dot(act[e], w.reshape(fh, dm)).astype(BF)

    def ahead(copies, es, end):
        for e in es:
            @pl.when(e + SLOTS < end)
            def _():
                start(copies(e + SLOTS))

    def forward(early, p, _):
        prev, now = group(p - 1), group(p)
        for e in prev:
            wait(down_early(e) if early else down(e))
        for e in now:
            wait(up(e))
        for e in prev:
            forward_out(e, early)
        for e in now:
            forward_hidden(e)
        if not early:
            ahead(down, prev, late)
        ahead(up, now, el)
        return 0

    for e in group(0):
        wait(up(e))
    for e in group(0):
        forward_hidden(e)
    for e in group(0):
        start(up(e + SLOTS))
    lax.fori_loop(1, late // GROUP + 1, functools.partial(forward, False), 0)
    lax.fori_loop(late // GROUP + 1, groups, functools.partial(forward, True), 0)
    for e in range(el - SLOTS, el):
        start(down(e))
    for e in group(groups - 1):
        wait(down_early(e))
    for e in group(groups - 1):
        forward_out(e, True)

    def y_part(s, out):
        def columns(c):
            n = min(256, dm - c)
            z = _dot(gate3_t[s], o[:, rows_of(s), pl.ds(c, n)].reshape(el * ROWS, n))
            out[:, pl.ds(c, n)] = z[:td] + z[td:2 * td] + z[2 * td:]
        return [functools.partial(columns, c) for c in range(0, dm, 256)]

    def y_half(j, h):
        return y_own.at[j, pl.ds(h * half, half)]

    def far_send(j, h, i, k):
        sent.append(send(y_half(j, h), y_far.at[i], yf_s.at[i], yf_r.at[i], k))

    def far_sum(i, j, h):
        arrive(y_far.at[i], yf_s.at[i], yf_r.at[i])
        return y_half(j, h)[...] + y_far[i]

    def dispatch_dy(s):
        gate = gates_of(s)
        dgt = []
        part = el // PARTS

        def rows(h):
            es = slice(h * part, (h + 1) * part)
            hot = onehot[s, h * part * ROWS:(h + 1) * part * ROWS, :]
            d = _dot(hot, dy_all[s])
            hot = hot.astype(F32)
            os = o[es, rows_of(s), :].reshape(part * ROWS, dm).astype(F32)
            dg = jnp.sum(d * os, axis=1, keepdims=True)
            dgt.append(jnp.sum((hot * dg).reshape(part, ROWS, td), axis=1))
            g = jnp.broadcast_to(gate[es][:, None, :], (part, ROWS, td)).reshape(part * ROWS, td)
            g = jnp.sum(hot * g, axis=1, keepdims=True)
            q[es, rows_of(s), :] = (g * d).astype(BF).reshape(part, ROWS, dm)

        def finish():
            total = jnp.concatenate(dgt, axis=0)
            for j in range(top):
                m = route_all[s, j:j + 1, :] == experts
                dg_send[s, j:j + 1, :] = jnp.sum(jnp.where(m, total, 0.0), axis=0, keepdims=True)

        return [functools.partial(rows, h) for h in range(PARTS)] + [finish]

    def together(y_steps, d_steps):
        each = -(-len(d_steps) // len(y_steps))
        for i, step in enumerate(y_steps):
            step()
            for d_step in d_steps[i * each:(i + 1) * each]:
                d_step()

    chip = []
    for i, k in enumerate((0, 1, 2, 4, 6, 3, 5, 7)):
        j = i % 4
        if i == 1:
            arrive(dy_all.at[peer(1)[1]], ys_sem.at[1], yr_sem.at[peer(1)[1]])
        if i == 2:
            for n in (2, 4, 6):
                s = peer(n)[1]
                arrive(dy_all.at[s], ys_sem.at[n], yr_sem.at[s])
                sent.append(send(dy_all.at[s], dy_all.at[s], ys_sem.at[n + 1], yr_sem.at[s], 1))
        if i == 5:
            for n in (3, 5, 7):
                s = peer(n)[1]
                arrive(dy_all.at[s], ys_sem.at[n], yr_sem.at[s])
        to_chip = i < 4
        together(y_part(peer(2 * j + 1 if to_chip else 2 * j)[1], (y_send if to_chip else y_own).at[j]), dispatch_dy(peer(k)[1]))
        if to_chip:
            chip.append(send(y_send.at[j], y_chip.at[j], yc_s.at[j], yc_r.at[j], 1))
    for j in (3, 1, 2, 0):
        arrive(y_chip.at[j], yc_s.at[j], yc_r.at[j])
        y_own[j] = y_own[j] + y_chip[j]
        if j == 2:
            far_send(3, 0, 0, 2)
            far_send(3, 1, 1, 4)
            far_send(1, 0, 2, 2)
            far_send(2, 1, 3, 4)
    for k in range(n_src):
        s = peer(k)[1]
        if k:
            sent.append(send(dg_send.at[s], dg_all.at[me], gs_sem.at[k], gr_sem.at[me], k))
        else:
            dg_all[me] = dg_send[s]

    def backward_hidden(e):
        da = _dot(q[e], w2[e % SLOTS].reshape(fh, dm), DIM1).astype(BF).astype(F32)
        uf = u[e].astype(F32)
        vf = v[e].astype(F32)
        sg = jax.nn.sigmoid(uf)
        return (da * vf * sg * (1 + uf * (1 - sg))).astype(BF), (da * (uf * sg)).astype(BF)

    def backward_hiddens(es):
        for e, (du, dv) in [(e, backward_hidden(e)) for e in es]:
            u[e] = du
            v[e] = dv

    def backward_out(e):
        slot = e % SLOTS
        o[e] = (_dot(u[e], w1[slot], DIM1) + _dot(v[e], w3[slot], DIM1)).astype(BF)

    def refill(copies, es):
        for e in es:
            @pl.when(e >= SLOTS)
            def _():
                start(copies(e - SLOTS))

    def ready(copies, es):
        for e in es:
            @pl.when(e < el - SLOTS)
            def _():
                wait(copies(e))

    def down_group(p):
        return [el - 1 - (p * GROUP + i) for i in range(GROUP)]

    def backward(p, _):
        prev, now = down_group(p - 1), down_group(p)
        ready(up, prev)
        for e in now:
            wait(down(e))
        for e in prev:
            backward_out(e)
        backward_hiddens(now)
        refill(up, prev)
        refill(down, now)
        return 0

    for e in down_group(0):
        wait(down(e))
    backward_hiddens(down_group(0))
    refill(down, down_group(0))
    lax.fori_loop(1, groups, backward, 0)
    ready(up, down_group(groups - 1))
    for e in down_group(groups - 1):
        backward_out(e)

    for k in range(1, n_src):
        s = peer(k)[1]
        arrive(dg_all.at[s], gs_sem.at[k], gr_sem.at[s])
    for c in chip:
        c.wait_send()

    def dx_part(s):
        return _dot(onehot_t[s], o[:, rows_of(s), :].reshape(el * ROWS, dm))

    for j in range(4):
        y_send[j] = dx_part(peer(2 * j + 1)[1])
        sent.append(send(y_send.at[j], y_chip.at[j], dc_s.at[j], dc_r.at[j], 1))
    d_own = (dx_here, to_x.at[pl.ds(0, td)], to_y.at[pl.ds(0, td)], to_xy)
    for j in range(4):
        d_own[j][...] = dx_part(peer(2 * j)[1])

    to_y[pl.ds(td, half), :] = far_sum(0, 2, 0)
    to_x[pl.ds(td, half), :] = far_sum(1, 1, 1)
    y_here[pl.ds(0, half), :] = far_sum(2, 0, 0)
    y_here[pl.ds(half, half), :] = far_sum(3, 0, 1)
    dg_out[...] = jnp.sum(dg_all[...], axis=0)

    for j in range(4):
        arrive(y_chip.at[j], dc_s.at[j], dc_r.at[j])
        d_own[j][...] = d_own[j][...] + y_chip[j]

    for c in sent:
        c.wait_send()


def _grad_kernel(xg, q, act, du, dv, dg, dw1, dw3, dw2, dg_out):
    for i in range(xg.shape[0]):
        dw1[i] = _dot(xg[i], du[i], DIM0)
        dw3[i] = _dot(xg[i], dv[i], DIM0)
        dw2[i] = _dot(act[i], q[i], DIM0)
    dg_out[...] = dg[...]


def _finish_kernel(y_here, dx_here, from_x, from_y, from_xy, y, dx):
    td = y.shape[0]
    half = td // 2
    dx[...] = (dx_here[...] + from_x[:td, :] + from_y[:td, :] + from_xy[...]).astype(BF)
    y[:half, :] = (y_here[:half, :] + from_y[td:, :]).astype(BF)
    y[half:, :] = (y_here[half:, :] + from_x[td:, :]).astype(BF)


def solution(mesh):
    ep = ('row', 'col', 'core')
    n_src = mesh.shape['row'] * mesh.shape['col'] * mesh.shape['core']
    tspec = P(('dp',) + ep, None)
    wspec = P(ep, None, None)
    gspec = P(('dp',) + ep, None, None)

    def body(x, route_idx, gates, w1, w3, w2, dy):
        td, top = route_idx.shape
        el, dm, fh = w1.shape
        er = n_src * ROWS
        sds = jax.ShapeDtypeStruct
        vmem = pltpu.VMEM
        dma = pltpu.SemaphoreType.DMA
        block = (td, dm)
        small = (n_src, top, td)
        whole = pl.BlockSpec(memory_space=pltpu.VMEM)
        flops = 2 * el * er * dm * fh * 6
        xg, q, act, du, dv, dg, y_here, dx_here, to_x, to_y, to_xy = pl.pallas_call(
            _core_kernel,
            name='moe_core',
            out_shape=[vmem((el, er, dm), BF), vmem((el, er, dm), BF)] + [vmem((el, er, fh), BF)] * 3
            + [vmem((top, td), F32), vmem(block, F32), vmem(block, F32)]
            + [vmem((td + td // 2, dm), F32)] * 2 + [vmem(block, F32)],
            in_specs=[ANY] * 7,
            out_specs=[whole] * 11,
            scratch_shapes=[
                vmem((n_src,) + block, BF), vmem((n_src,) + block, BF), vmem(small, jnp.int32), vmem(small, F32),
                vmem((el, er, dm), BF),
                vmem((n_src, el * ROWS, td), BF), vmem((n_src, td, el * ROWS), BF), vmem((n_src, 3 * td, el * ROWS), BF),
                vmem((SLOTS, dm, fh), BF), vmem((SLOTS, dm, fh), BF), vmem((SLOTS, fh // er, er, dm), BF),
                vmem((4,) + block, F32), vmem((4,) + block, F32), vmem((4,) + block, F32), vmem((4, td // 2, dm), F32),
                vmem(small, F32), vmem(small, F32),
                dma((4,)), dma((3, SLOTS)), dma((el,)),
                dma((16,)), dma((16,)), dma((8,)), dma((8,)), dma((8,)), dma((8,)), dma((8,)), dma((8,)),
                dma((4,)), dma((4,)), dma((4,)), dma((4,)), dma((4,)), dma((4,)), dma((8,)), dma((8,)),
            ],
            compiler_params=pltpu.CompilerParams(collective_id=0, has_side_effects=True, vmem_limit_bytes=CORE_VMEM << 20),
            cost_estimate=pl.CostEstimate(flops=flops, bytes_accessed=88 << 20, transcendentals=0),
        )(x, dy, route_idx.T, gates.T, w1, w3, w2.reshape(el, fh // er, er, dm))

        def swap(a, k):
            return lax.ppermute(a, ep, [(i, i ^ k) for i in range(n_src)])

        from_xy, from_x, from_y = swap(to_xy, 6), swap(to_x, 2), swap(to_y, 4)
        per = 2
        spec = lambda a, b: pl.BlockSpec((per, a, b), lambda i: (i, 0, 0))
        once = lambda a, b: pl.BlockSpec((a, b), lambda i: (0, 0))

        dw1, dw3, dw2, dg = pl.pallas_call(
            _grad_kernel,
            name='moe_grad',
            grid=(el // per,),
            out_shape=[sds((el, dm, fh), F32), sds((el, dm, fh), F32), sds((el, fh, dm), F32), sds((top, td), F32)],
            in_specs=[spec(er, dm), spec(er, dm), spec(er, fh), spec(er, fh), spec(er, fh), once(top, td)],
            out_specs=[spec(dm, fh), spec(dm, fh), spec(fh, dm), once(top, td)],
            compiler_params=pltpu.CompilerParams(vmem_limit_bytes=GRAD_VMEM << 20),
            cost_estimate=pl.CostEstimate(flops=2 * el * er * dm * fh * 3, bytes_accessed=90 << 20, transcendentals=0),
        )(xg, q, act, du, dv, dg)
        y, dx = pl.pallas_call(
            _finish_kernel,
            name='moe_finish',
            out_shape=[sds(block, BF), sds(block, BF)],
            in_specs=[whole] * 5,
            out_specs=[whole] * 2,
            compiler_params=pltpu.CompilerParams(vmem_limit_bytes=FINISH_VMEM << 20),
        )(y_here, dx_here, from_x, from_y, from_xy)
        return y, dx, dg.T, dw1, dw3, dw2

    return jax.shard_map(body, mesh=mesh, in_specs=(tspec, tspec, tspec, wspec, wspec, wspec, tspec),
                         out_specs=(tspec, tspec, tspec, gspec, gspec, gspec), check_vma=False)
```

```python
import functools

import jax
import jax.numpy as jnp
from jax import lax
from jax.experimental import pallas as pl
from jax.experimental.pallas import tpu as pltpu
from jax.sharding import PartitionSpec as P

MESH = pl.DeviceIdType.MESH
F32 = jnp.float32
BF = jnp.bfloat16
ROWS = 16
SLOTS = 12
CORE_VMEM = 41
GRAD_VMEM = 14
FINISH_VMEM = 6
GROUP = 4
PARTS = 4
DIM0 = (((0,), (0,)), ((), ()))
DIM1 = (((1,), (1,)), ((), ()))
ANY = pl.BlockSpec(memory_space=pl.ANY)


def _dot(a, b, dims=(((1,), (0,)), ((), ()))):
    return lax.dot_general(a, b, dims, preferred_element_type=F32)


def _core_kernel(x_hbm, dy_hbm, route_hbm, gate_hbm, w1_hbm, w3_hbm, w2_hbm,
                 xg, q, act, u, v, dg_out, y_here, dx_here, to_x, to_y, to_xy,
                 x_all, dy_all, route_all, gate_all, o, onehot, onehot_t, gate3_t,
                 w1, w3, w2, y_send, y_own, y_chip, y_far, dg_send, dg_all,
                 in_sem, w_sem, e_sem,
                 xs_sem, xr_sem, ys_sem, yr_sem, ts_sem, tr_sem, gts_sem, gtr_sem,
                 yc_s, yc_r, yf_s, yf_r, dc_s, dc_r, gs_sem, gr_sem):
    row, col, core = lax.axis_index('row'), lax.axis_index('col'), lax.axis_index('core')
    el, dm, fh = w1_hbm.shape
    late = el - el // w2_hbm.shape[1]
    td = x_hbm.shape[0]
    top = route_hbm.shape[0]
    n_src = x_all.shape[0]

    def peer(k):
        r = 1 - row if k & 4 else row
        c = 1 - col if k & 2 else col
        h = 1 - core if k & 1 else core
        return {'row': r, 'col': c, 'core': h}, r * 4 + c * 2 + h

    me = peer(0)[1]

    def start(copies):
        for c in copies:
            c.start()

    def wait(copies):
        for c in copies:
            c.wait()

    own = [pltpu.make_async_copy(a, b.at[me], in_sem.at[i])
           for i, (a, b) in enumerate(((route_hbm, route_all), (gate_hbm, gate_all), (x_hbm, x_all), (dy_hbm, dy_all)))]
    start(own)

    def up(e):
        slot = e % SLOTS
        return [pltpu.make_async_copy(a.at[e], b.at[slot], w_sem.at[j, slot])
                for j, (a, b) in enumerate(((w1_hbm, w1), (w3_hbm, w3)))]

    def down(e):
        return [pltpu.make_async_copy(w2_hbm.at[e], w2.at[e % SLOTS], w_sem.at[2, e % SLOTS])]

    def down_early(e):
        n = w2_hbm.shape[1]
        return [pltpu.make_async_copy(w2_hbm.at[e], q.at[pl.ds((e - late) * n, n)], e_sem.at[e - late])]

    barrier = pltpu.get_barrier_semaphore()
    for k in range(1, n_src):
        pl.semaphore_signal(barrier, inc=1, device_id=peer(k)[0], device_id_type=MESH)
    for e in range(SLOTS):
        start(up(e) + down(e))
    for e in range(late, el):
        start(down_early(e))
    pl.semaphore_wait(barrier, n_src - 1)

    def send(src, dst, s_sem, r_sem, k):
        c = pltpu.make_async_remote_copy(src_ref=src, dst_ref=dst, send_sem=s_sem, recv_sem=r_sem,
                                         device_id=peer(k)[0], device_id_type=MESH)
        c.start()
        return c

    def arrive(dst, s_sem, r_sem):
        pltpu.make_async_remote_copy(src_ref=dst, dst_ref=dst, send_sem=s_sem, recv_sem=r_sem,
                                     device_id=peer(1)[0], device_id_type=MESH).wait_recv()

    sent = []
    wait(own[:2])
    for k in range(1, n_src):
        sent.append(send(route_all.at[me], route_all.at[me], ts_sem.at[k], tr_sem.at[me], k))
        sent.append(send(gate_all.at[me], gate_all.at[me], gts_sem.at[k], gtr_sem.at[me], k))
    wait(own[2:])
    half = td // 2

    def x_half(s, h):
        return x_all.at[s, pl.ds(h * half, half)]

    def x_send(s, h, k):
        i = len(x_sent)
        x_sent.append(send(x_half(s, h), x_half(s, h), xs_sem.at[i], xr_sem.at[2 * s + h], k))

    def x_wait(s, h):
        arrive(x_half(s, h), xs_sem.at[0], xr_sem.at[2 * s + h])

    x_sent = []
    for h in range(2):
        x_send(me, h, 2)
        x_send(me, 1 - h, 4)
    for h in range(2):
        x_send(me, h, 1)

    for k in range(1, n_src):
        s = peer(k)[1]
        arrive(route_all.at[s], ts_sem.at[k], tr_sem.at[s])
        arrive(gate_all.at[s], gts_sem.at[k], gtr_sem.at[s])

    experts = lax.broadcasted_iota(jnp.int32, (el, td), 0) + me * el
    before = (lax.broadcasted_iota(jnp.int32, (td, td), 0) < lax.broadcasted_iota(jnp.int32, (td, td), 1))
    before = jnp.where(before, 1.0, 0.0).astype(BF)
    place = lax.broadcasted_iota(jnp.int32, (el, ROWS, td), 1).astype(F32)

    def gates_of(s):
        gate = jnp.zeros((el, td), F32)
        for j in range(top):
            gate = jnp.where(route_all[s, j:j + 1, :] == experts, gate_all[s, j:j + 1, :], gate)
        return gate

    def tables(s, _):
        hit = jnp.zeros((el, td), F32)
        for j in range(top):
            hit = jnp.where(route_all[s, j:j + 1, :] == experts, 1.0, hit)
        rank = jnp.where(hit > 0, _dot(hit.astype(BF), before), -1.0)
        sel = jnp.broadcast_to(rank[:, None, :], place.shape) == place
        hot = jnp.where(sel, 1.0, 0.0).reshape(el * ROWS, td)
        onehot[s] = hot.astype(BF)
        onehot_t[s] = hot.T.astype(BF)
        g = jnp.where(sel, jnp.broadcast_to(gates_of(s)[:, None, :], place.shape), 0.0)
        g = g.reshape(el * ROWS, td).T
        for i in range(3):
            part = g.astype(BF)
            gate3_t[s, i * td:(i + 1) * td, :] = part
            g = g - part.astype(F32)
        return 0

    lax.fori_loop(0, n_src, tables, 0)

    def rows_of(s):
        return pl.ds(pl.multiple_of(s * ROWS, ROWS), ROWS)

    def dispatch_x(k):
        s = peer(k)[1]
        xg[:, rows_of(s), :] = _dot(onehot[s], x_all[s]).astype(BF).reshape(el, ROWS, dm)

    near_x, near_y, diagonal = peer(2)[1], peer(4)[1], peer(6)[1]
    x_wait(near_x, 0)
    x_send(near_x, 0, 4)
    x_send(near_x, 0, 1)
    x_wait(near_y, 1)
    x_send(near_y, 1, 2)
    x_send(near_y, 1, 1)
    dispatch_x(0)
    for h in range(2):
        x_wait(peer(1)[1], h)
    dispatch_x(1)
    x_wait(near_x, 1)
    x_send(near_x, 1, 1)
    x_wait(near_y, 0)
    x_send(near_y, 0, 1)
    for k in (2, 4):
        dispatch_x(k)
    for k in (3, 5):
        for h in range(2):
            x_wait(peer(k)[1], h)
        dispatch_x(k)
    for h in range(2):
        x_wait(diagonal, h)
        x_send(diagonal, h, 1)
    for k in (2, 4, 6, 1):
        sent.append(send(dy_all.at[me], dy_all.at[me], ys_sem.at[k], yr_sem.at[me], k))
    dispatch_x(6)
    for h in range(2):
        x_wait(peer(7)[1], h)
    dispatch_x(7)
    sent += x_sent

    def group(p):
        return [p * GROUP + i for i in range(GROUP)]

    groups = el // GROUP

    def forward_hidden(e):
        slot = e % SLOTS
        xe = xg[e]
        ue = _dot(xe, w1[slot]).astype(BF)
        ve = _dot(xe, w3[slot]).astype(BF)
        u[e] = ue
        v[e] = ve
        uf = ue.astype(F32)
        act[e] = (uf * jax.nn.sigmoid(uf) * ve.astype(F32)).astype(BF)

    def forward_out(e, early):
        n = w2_hbm.shape[1]
        w = q[pl.ds((e - late) * n, n)] if early else w2[e % SLOTS]
        o[e] = _dot(act[e], w.reshape(fh, dm)).astype(BF)

    def ahead(copies, es, end):
        for e in es:
            @pl.when(e + SLOTS < end)
            def _():
                start(copies(e + SLOTS))

    def forward(early, p, _):
        prev, now = group(p - 1), group(p)
        for e in prev:
            wait(down_early(e) if early else down(e))
        for e in now:
            wait(up(e))
        for e in prev:
            forward_out(e, early)
        for e in now:
            forward_hidden(e)
        if not early:
            ahead(down, prev, late)
        ahead(up, now, el)
        return 0

    for e in group(0):
        wait(up(e))
    for e in group(0):
        forward_hidden(e)
    for e in group(0):
        start(up(e + SLOTS))
    lax.fori_loop(1, late // GROUP + 1, functools.partial(forward, False), 0)
    lax.fori_loop(late // GROUP + 1, groups, functools.partial(forward, True), 0)
    for e in range(el - SLOTS, el):
        start(down(e))
    for e in group(groups - 1):
        wait(down_early(e))
    for e in group(groups - 1):
        forward_out(e, True)

    def y_part(s, out):
        def columns(c):
            n = min(256, dm - c)
            z = _dot(gate3_t[s], o[:, rows_of(s), pl.ds(c, n)].reshape(el * ROWS, n))
            out[:, pl.ds(c, n)] = z[:td] + z[td:2 * td] + z[2 * td:]
        return [functools.partial(columns, c) for c in range(0, dm, 256)]

    def y_half(j, h):
        return y_own.at[j, pl.ds(h * half, half)]

    def far_send(j, h, i, k):
        sent.append(send(y_half(j, h), y_far.at[i], yf_s.at[i], yf_r.at[i], k))

    def far_sum(i, j, h):
        arrive(y_far.at[i], yf_s.at[i], yf_r.at[i])
        return y_half(j, h)[...] + y_far[i]

    def dispatch_dy(s):
        gate = gates_of(s)
        dgt = []
        part = el // PARTS

        def rows(h):
            es = slice(h * part, (h + 1) * part)
            hot = onehot[s, h * part * ROWS:(h + 1) * part * ROWS, :]
            d = _dot(hot, dy_all[s])
            hot = hot.astype(F32)
            os = o[es, rows_of(s), :].reshape(part * ROWS, dm).astype(F32)
            dg = jnp.sum(d * os, axis=1, keepdims=True)
            dgt.append(jnp.sum((hot * dg).reshape(part, ROWS, td), axis=1))
            g = jnp.broadcast_to(gate[es][:, None, :], (part, ROWS, td)).reshape(part * ROWS, td)
            g = jnp.sum(hot * g, axis=1, keepdims=True)
            q[es, rows_of(s), :] = (g * d).astype(BF).reshape(part, ROWS, dm)

        def finish():
            total = jnp.concatenate(dgt, axis=0)
            for j in range(top):
                m = route_all[s, j:j + 1, :] == experts
                dg_send[s, j:j + 1, :] = jnp.sum(jnp.where(m, total, 0.0), axis=0, keepdims=True)

        return [functools.partial(rows, h) for h in range(PARTS)] + [finish]

    def together(y_steps, d_steps):
        each = -(-len(d_steps) // len(y_steps))
        for i, step in enumerate(y_steps):
            step()
            for d_step in d_steps[i * each:(i + 1) * each]:
                d_step()

    chip = []
    for i, ks in enumerate(((0,), (1,), (), (2,), (4,), (6,), (3, 5), (7,))):
        j = i % 4
        if 1 in ks:
            arrive(dy_all.at[peer(1)[1]], ys_sem.at[1], yr_sem.at[peer(1)[1]])
        if 2 in ks:
            for n in (2, 4, 6):
                s = peer(n)[1]
                arrive(dy_all.at[s], ys_sem.at[n], yr_sem.at[s])
                sent.append(send(dy_all.at[s], dy_all.at[s], ys_sem.at[n + 1], yr_sem.at[s], 1))
        if 3 in ks:
            for n in (3, 5, 7):
                s = peer(n)[1]
                arrive(dy_all.at[s], ys_sem.at[n], yr_sem.at[s])
        to_chip = i < 4
        together(y_part(peer(2 * j + 1 if to_chip else 2 * j)[1], (y_send if to_chip else y_own).at[j]), [step for k in ks for step in dispatch_dy(peer(k)[1])])
        if to_chip:
            chip.append(send(y_send.at[j], y_chip.at[j], yc_s.at[j], yc_r.at[j], 1))
    for j in (3, 1, 2, 0):
        arrive(y_chip.at[j], yc_s.at[j], yc_r.at[j])
        y_own[j] = y_own[j] + y_chip[j]
        if j == 2:
            far_send(3, 0, 0, 2)
            far_send(3, 1, 1, 4)
            far_send(1, 0, 2, 2)
            far_send(2, 1, 3, 4)
    for k in range(n_src):
        s = peer(k)[1]
        if k:
            sent.append(send(dg_send.at[s], dg_all.at[me], gs_sem.at[k], gr_sem.at[me], k))
        else:
            dg_all[me] = dg_send[s]

    def backward_hidden(e):
        da = _dot(q[e], w2[e % SLOTS].reshape(fh, dm), DIM1).astype(BF).astype(F32)
        uf = u[e].astype(F32)
        vf = v[e].astype(F32)
        sg = jax.nn.sigmoid(uf)
        return (da * vf * sg * (1 + uf * (1 - sg))).astype(BF), (da * (uf * sg)).astype(BF)

    def backward_hiddens(es):
        for e, (du, dv) in [(e, backward_hidden(e)) for e in es]:
            u[e] = du
            v[e] = dv

    def backward_out(e):
        slot = e % SLOTS
        o[e] = (_dot(u[e], w1[slot], DIM1) + _dot(v[e], w3[slot], DIM1)).astype(BF)

    def refill(copies, es):
        for e in es:
            @pl.when(e >= SLOTS)
            def _():
                start(copies(e - SLOTS))

    def ready(copies, es):
        for e in es:
            @pl.when(e < el - SLOTS)
            def _():
                wait(copies(e))

    def down_group(p):
        return [el - 1 - (p * GROUP + i) for i in range(GROUP)]

    def backward(p, _):
        prev, now = down_group(p - 1), down_group(p)
        ready(up, prev)
        for e in now:
            wait(down(e))
        for e in prev:
            backward_out(e)
        backward_hiddens(now)
        refill(up, prev)
        refill(down, now)
        return 0

    for e in down_group(0):
        wait(down(e))
    backward_hiddens(down_group(0))
    refill(down, down_group(0))
    lax.fori_loop(1, groups, backward, 0)
    ready(up, down_group(groups - 1))
    for e in down_group(groups - 1):
        backward_out(e)

    for k in range(1, n_src):
        s = peer(k)[1]
        arrive(dg_all.at[s], gs_sem.at[k], gr_sem.at[s])
    for c in chip:
        c.wait_send()

    def dx_part(s):
        return _dot(onehot_t[s], o[:, rows_of(s), :].reshape(el * ROWS, dm))

    for j in range(4):
        y_send[j] = dx_part(peer(2 * j + 1)[1])
        sent.append(send(y_send.at[j], y_chip.at[j], dc_s.at[j], dc_r.at[j], 1))
    d_own = (dx_here, to_x.at[pl.ds(0, td)], to_y.at[pl.ds(0, td)], to_xy)
    for j in range(4):
        d_own[j][...] = dx_part(peer(2 * j)[1])

    to_y[pl.ds(td, half), :] = far_sum(0, 2, 0)
    to_x[pl.ds(td, half), :] = far_sum(1, 1, 1)
    y_here[pl.ds(0, half), :] = far_sum(2, 0, 0)
    y_here[pl.ds(half, half), :] = far_sum(3, 0, 1)
    dg_out[...] = jnp.sum(dg_all[...], axis=0)

    for j in range(4):
        arrive(y_chip.at[j], dc_s.at[j], dc_r.at[j])
        d_own[j][...] = d_own[j][...] + y_chip[j]

    for c in sent:
        c.wait_send()


def _grad_kernel(xg, q, act, du, dv, dg, dw1, dw3, dw2, dg_out):
    for i in range(xg.shape[0]):
        dw1[i] = _dot(xg[i], du[i], DIM0)
        dw3[i] = _dot(xg[i], dv[i], DIM0)
        dw2[i] = _dot(act[i], q[i], DIM0)
    dg_out[...] = dg[...]


def _finish_kernel(y_here, dx_here, from_x, from_y, from_xy, y, dx):
    td = y.shape[0]
    half = td // 2
    dx[...] = (dx_here[...] + from_x[:td, :] + from_y[:td, :] + from_xy[...]).astype(BF)
    y[:half, :] = (y_here[:half, :] + from_y[td:, :]).astype(BF)
    y[half:, :] = (y_here[half:, :] + from_x[td:, :]).astype(BF)


def solution(mesh):
    ep = ('row', 'col', 'core')
    n_src = mesh.shape['row'] * mesh.shape['col'] * mesh.shape['core']
    tspec = P(('dp',) + ep, None)
    wspec = P(ep, None, None)
    gspec = P(('dp',) + ep, None, None)

    def body(x, route_idx, gates, w1, w3, w2, dy):
        td, top = route_idx.shape
        el, dm, fh = w1.shape
        er = n_src * ROWS
        sds = jax.ShapeDtypeStruct
        vmem = pltpu.VMEM
        dma = pltpu.SemaphoreType.DMA
        block = (td, dm)
        small = (n_src, top, td)
        whole = pl.BlockSpec(memory_space=pltpu.VMEM)
        flops = 2 * el * er * dm * fh * 6
        xg, q, act, du, dv, dg, y_here, dx_here, to_x, to_y, to_xy = pl.pallas_call(
            _core_kernel,
            name='moe_core',
            out_shape=[vmem((el, er, dm), BF), vmem((el, er, dm), BF)] + [vmem((el, er, fh), BF)] * 3
            + [vmem((top, td), F32), vmem(block, F32), vmem(block, F32)]
            + [vmem((td + td // 2, dm), F32)] * 2 + [vmem(block, F32)],
            in_specs=[ANY] * 7,
            out_specs=[whole] * 11,
            scratch_shapes=[
                vmem((n_src,) + block, BF), vmem((n_src,) + block, BF), vmem(small, jnp.int32), vmem(small, F32),
                vmem((el, er, dm), BF),
                vmem((n_src, el * ROWS, td), BF), vmem((n_src, td, el * ROWS), BF), vmem((n_src, 3 * td, el * ROWS), BF),
                vmem((SLOTS, dm, fh), BF), vmem((SLOTS, dm, fh), BF), vmem((SLOTS, fh // er, er, dm), BF),
                vmem((4,) + block, F32), vmem((4,) + block, F32), vmem((4,) + block, F32), vmem((4, td // 2, dm), F32),
                vmem(small, F32), vmem(small, F32),
                dma((4,)), dma((3, SLOTS)), dma((el,)),
                dma((16,)), dma((16,)), dma((8,)), dma((8,)), dma((8,)), dma((8,)), dma((8,)), dma((8,)),
                dma((4,)), dma((4,)), dma((4,)), dma((4,)), dma((4,)), dma((4,)), dma((8,)), dma((8,)),
            ],
            compiler_params=pltpu.CompilerParams(collective_id=0, has_side_effects=True, vmem_limit_bytes=CORE_VMEM << 20),
            cost_estimate=pl.CostEstimate(flops=flops, bytes_accessed=88 << 20, transcendentals=0),
        )(x, dy, route_idx.T, gates.T, w1, w3, w2.reshape(el, fh // er, er, dm))

        def swap(a, k):
            return lax.ppermute(a, ep, [(i, i ^ k) for i in range(n_src)])

        from_xy, from_x, from_y = swap(to_xy, 6), swap(to_x, 2), swap(to_y, 4)
        per = 2
        spec = lambda a, b: pl.BlockSpec((per, a, b), lambda i: (i, 0, 0))
        once = lambda a, b: pl.BlockSpec((a, b), lambda i: (0, 0))

        dw1, dw3, dw2, dg = pl.pallas_call(
            _grad_kernel,
            name='moe_grad',
            grid=(el // per,),
            out_shape=[sds((el, dm, fh), F32), sds((el, dm, fh), F32), sds((el, fh, dm), F32), sds((top, td), F32)],
            in_specs=[spec(er, dm), spec(er, dm), spec(er, fh), spec(er, fh), spec(er, fh), once(top, td)],
            out_specs=[spec(dm, fh), spec(dm, fh), spec(fh, dm), once(top, td)],
            compiler_params=pltpu.CompilerParams(vmem_limit_bytes=GRAD_VMEM << 20),
            cost_estimate=pl.CostEstimate(flops=2 * el * er * dm * fh * 3, bytes_accessed=90 << 20, transcendentals=0),
        )(xg, q, act, du, dv, dg)
        y, dx = pl.pallas_call(
            _finish_kernel,
            name='moe_finish',
            out_shape=[sds(block, BF), sds(block, BF)],
            in_specs=[whole] * 5,
            out_specs=[whole] * 2,
            compiler_params=pltpu.CompilerParams(vmem_limit_bytes=FINISH_VMEM << 20),
        )(y_here, dx_here, from_x, from_y, from_xy)
        return y, dx, dg.T, dw1, dw3, dw2

    return jax.shard_map(body, mesh=mesh, in_specs=(tspec, tspec, tspec, wspec, wspec, wspec, tspec),
                         out_specs=(tspec, tspec, tspec, gspec, gspec, gspec), check_vma=False)
```

```python
import functools

import jax
import jax.numpy as jnp
from jax import lax
from jax.experimental import pallas as pl
from jax.experimental.pallas import tpu as pltpu
from jax.sharding import PartitionSpec as P

MESH = pl.DeviceIdType.MESH
F32 = jnp.float32
BF = jnp.bfloat16
ROWS = 16
SLOTS = 12
CORE_VMEM = 41
GRAD_VMEM = 14
FINISH_VMEM = 6
GROUP = 4
PARTS = 4
DIM0 = (((0,), (0,)), ((), ()))
DIM1 = (((1,), (1,)), ((), ()))
ANY = pl.BlockSpec(memory_space=pl.ANY)


def _dot(a, b, dims=(((1,), (0,)), ((), ()))):
    return lax.dot_general(a, b, dims, preferred_element_type=F32)


def _core_kernel(x_hbm, dy_hbm, route_hbm, gate_hbm, w1_hbm, w3_hbm, w2_hbm,
                 xg, q, act, u, v, dg_out, y_here, dx_here, to_x, to_y, to_xy,
                 x_all, dy_all, route_all, gate_all, o, onehot, onehot_t, gate3_t,
                 w1, w3, w2, y_send, y_own, y_chip, y_far, dg_send, dg_all,
                 in_sem, w_sem, e_sem,
                 xs_sem, xr_sem, ys_sem, yr_sem, ts_sem, tr_sem, gts_sem, gtr_sem,
                 yc_s, yc_r, yf_s, yf_r, dc_s, dc_r, gs_sem, gr_sem):
    row, col, core = lax.axis_index('row'), lax.axis_index('col'), lax.axis_index('core')
    el, dm, fh = w1_hbm.shape
    late = el - el // w2_hbm.shape[1]
    td = x_hbm.shape[0]
    top = route_hbm.shape[0]
    n_src = x_all.shape[0]

    def peer(k):
        r = 1 - row if k & 4 else row
        c = 1 - col if k & 2 else col
        h = 1 - core if k & 1 else core
        return {'row': r, 'col': c, 'core': h}, r * 4 + c * 2 + h

    me = peer(0)[1]

    def start(copies):
        for c in copies:
            c.start()

    def wait(copies):
        for c in copies:
            c.wait()

    own = [pltpu.make_async_copy(a, b.at[me], in_sem.at[i])
           for i, (a, b) in enumerate(((route_hbm, route_all), (gate_hbm, gate_all), (x_hbm, x_all), (dy_hbm, dy_all)))]
    start(own)

    def up(e):
        slot = e % SLOTS
        return [pltpu.make_async_copy(a.at[e], b.at[slot], w_sem.at[j, slot])
                for j, (a, b) in enumerate(((w1_hbm, w1), (w3_hbm, w3)))]

    def down(e):
        return [pltpu.make_async_copy(w2_hbm.at[e], w2.at[e % SLOTS], w_sem.at[2, e % SLOTS])]

    def down_early(e):
        n = w2_hbm.shape[1]
        return [pltpu.make_async_copy(w2_hbm.at[e], q.at[pl.ds((e - late) * n, n)], e_sem.at[e - late])]

    barrier = pltpu.get_barrier_semaphore()
    for k in range(1, n_src):
        pl.semaphore_signal(barrier, inc=1, device_id=peer(k)[0], device_id_type=MESH)
    for e in range(SLOTS):
        start(up(e) + down(e))
    for e in range(late, el):
        start(down_early(e))
    pl.semaphore_wait(barrier, n_src - 1)

    def send(src, dst, s_sem, r_sem, k):
        c = pltpu.make_async_remote_copy(src_ref=src, dst_ref=dst, send_sem=s_sem, recv_sem=r_sem,
                                         device_id=peer(k)[0], device_id_type=MESH)
        c.start()
        return c

    def arrive(dst, s_sem, r_sem):
        pltpu.make_async_remote_copy(src_ref=dst, dst_ref=dst, send_sem=s_sem, recv_sem=r_sem,
                                     device_id=peer(1)[0], device_id_type=MESH).wait_recv()

    sent = []
    wait(own[:2])
    for k in range(1, n_src):
        sent.append(send(route_all.at[me], route_all.at[me], ts_sem.at[k], tr_sem.at[me], k))
        sent.append(send(gate_all.at[me], gate_all.at[me], gts_sem.at[k], gtr_sem.at[me], k))
    wait(own[2:])
    half = td // 2

    def x_half(s, h):
        return x_all.at[s, pl.ds(h * half, half)]

    def x_send(s, h, k):
        i = len(x_sent)
        x_sent.append(send(x_half(s, h), x_half(s, h), xs_sem.at[i], xr_sem.at[2 * s + h], k))

    def x_wait(s, h):
        arrive(x_half(s, h), xs_sem.at[0], xr_sem.at[2 * s + h])

    x_sent = []
    for h in range(2):
        x_send(me, h, 2)
        x_send(me, 1 - h, 4)
    for h in range(2):
        x_send(me, h, 1)

    for k in range(1, n_src):
        s = peer(k)[1]
        arrive(route_all.at[s], ts_sem.at[k], tr_sem.at[s])
        arrive(gate_all.at[s], gts_sem.at[k], gtr_sem.at[s])

    experts = lax.broadcasted_iota(jnp.int32, (el, td), 0) + me * el
    before = (lax.broadcasted_iota(jnp.int32, (td, td), 0) < lax.broadcasted_iota(jnp.int32, (td, td), 1))
    before = jnp.where(before, 1.0, 0.0).astype(BF)
    place = lax.broadcasted_iota(jnp.int32, (el, ROWS, td), 1).astype(F32)

    def gates_of(s):
        gate = jnp.zeros((el, td), F32)
        for j in range(top):
            gate = jnp.where(route_all[s, j:j + 1, :] == experts, gate_all[s, j:j + 1, :], gate)
        return gate

    def tables(s, _):
        hit = jnp.zeros((el, td), F32)
        for j in range(top):
            hit = jnp.where(route_all[s, j:j + 1, :] == experts, 1.0, hit)
        rank = jnp.where(hit > 0, _dot(hit.astype(BF), before), -1.0)
        sel = jnp.broadcast_to(rank[:, None, :], place.shape) == place
        hot = jnp.where(sel, 1.0, 0.0).reshape(el * ROWS, td)
        onehot[s] = hot.astype(BF)
        onehot_t[s] = hot.T.astype(BF)
        g = jnp.where(sel, jnp.broadcast_to(gates_of(s)[:, None, :], place.shape), 0.0)
        g = g.reshape(el * ROWS, td).T
        for i in range(3):
            part = g.astype(BF)
            gate3_t[s, i * td:(i + 1) * td, :] = part
            g = g - part.astype(F32)
        return 0

    lax.fori_loop(0, n_src, tables, 0)

    def rows_of(s):
        return pl.ds(pl.multiple_of(s * ROWS, ROWS), ROWS)

    def dispatch_x(k):
        s = peer(k)[1]
        xg[:, rows_of(s), :] = _dot(onehot[s], x_all[s]).astype(BF).reshape(el, ROWS, dm)

    near_x, near_y, diagonal = peer(2)[1], peer(4)[1], peer(6)[1]
    x_wait(near_x, 0)
    x_send(near_x, 0, 4)
    x_send(near_x, 0, 1)
    x_wait(near_y, 1)
    x_send(near_y, 1, 2)
    x_send(near_y, 1, 1)
    dispatch_x(0)
    for h in range(2):
        x_wait(peer(1)[1], h)
    dispatch_x(1)
    x_wait(near_x, 1)
    x_send(near_x, 1, 1)
    x_wait(near_y, 0)
    x_send(near_y, 0, 1)
    for k in (2, 4):
        dispatch_x(k)
    for h in range(2):
        x_wait(peer(3)[1], h)
    dispatch_x(3)
    for h in range(2):
        x_wait(diagonal, h)
        x_send(diagonal, h, 1)
    for k in (2, 4, 6, 1):
        sent.append(send(dy_all.at[me], dy_all.at[me], ys_sem.at[k], yr_sem.at[me], k))
    for h in range(2):
        x_wait(peer(5)[1], h)
    dispatch_x(5)
    dispatch_x(6)
    for h in range(2):
        x_wait(peer(7)[1], h)
    dispatch_x(7)
    sent += x_sent

    def group(p):
        return [p * GROUP + i for i in range(GROUP)]

    groups = el // GROUP

    def forward_hidden(e):
        slot = e % SLOTS
        xe = xg[e]
        ue = _dot(xe, w1[slot]).astype(BF)
        ve = _dot(xe, w3[slot]).astype(BF)
        u[e] = ue
        v[e] = ve
        uf = ue.astype(F32)
        act[e] = (uf * jax.nn.sigmoid(uf) * ve.astype(F32)).astype(BF)

    def forward_out(e, early):
        n = w2_hbm.shape[1]
        w = q[pl.ds((e - late) * n, n)] if early else w2[e % SLOTS]
        o[e] = _dot(act[e], w.reshape(fh, dm)).astype(BF)

    def ahead(copies, es, end):
        for e in es:
            @pl.when(e + SLOTS < end)
            def _():
                start(copies(e + SLOTS))

    def forward(early, p, _):
        prev, now = group(p - 1), group(p)
        for e in prev:
            wait(down_early(e) if early else down(e))
        for e in now:
            wait(up(e))
        for e in prev:
            forward_out(e, early)
        for e in now:
            forward_hidden(e)
        if not early:
            ahead(down, prev, late)
        ahead(up, now, el)
        return 0

    for e in group(0):
        wait(up(e))
    for e in group(0):
        forward_hidden(e)
    for e in group(0):
        start(up(e + SLOTS))
    lax.fori_loop(1, late // GROUP + 1, functools.partial(forward, False), 0)
    lax.fori_loop(late // GROUP + 1, groups, functools.partial(forward, True), 0)
    for e in range(el - SLOTS, el):
        start(down(e))
    for e in group(groups - 1):
        wait(down_early(e))
    for e in group(groups - 1):
        forward_out(e, True)

    def y_part(s, out):
        def columns(c):
            n = min(256, dm - c)
            z = _dot(gate3_t[s], o[:, rows_of(s), pl.ds(c, n)].reshape(el * ROWS, n))
            out[:, pl.ds(c, n)] = z[:td] + z[td:2 * td] + z[2 * td:]
        return [functools.partial(columns, c) for c in range(0, dm, 256)]

    def y_half(j, h):
        return y_own.at[j, pl.ds(h * half, half)]

    def far_send(j, h, i, k):
        sent.append(send(y_half(j, h), y_far.at[i], yf_s.at[i], yf_r.at[i], k))

    def far_sum(i, j, h):
        arrive(y_far.at[i], yf_s.at[i], yf_r.at[i])
        return y_half(j, h)[...] + y_far[i]

    def dispatch_dy(s):
        gate = gates_of(s)
        dgt = []
        part = el // PARTS

        def rows(h):
            es = slice(h * part, (h + 1) * part)
            hot = onehot[s, h * part * ROWS:(h + 1) * part * ROWS, :]
            d = _dot(hot, dy_all[s])
            hot = hot.astype(F32)
            os = o[es, rows_of(s), :].reshape(part * ROWS, dm).astype(F32)
            dg = jnp.sum(d * os, axis=1, keepdims=True)
            dgt.append(jnp.sum((hot * dg).reshape(part, ROWS, td), axis=1))
            g = jnp.broadcast_to(gate[es][:, None, :], (part, ROWS, td)).reshape(part * ROWS, td)
            g = jnp.sum(hot * g, axis=1, keepdims=True)
            q[es, rows_of(s), :] = (g * d).astype(BF).reshape(part, ROWS, dm)

        def finish():
            total = jnp.concatenate(dgt, axis=0)
            for j in range(top):
                m = route_all[s, j:j + 1, :] == experts
                dg_send[s, j:j + 1, :] = jnp.sum(jnp.where(m, total, 0.0), axis=0, keepdims=True)

        return [functools.partial(rows, h) for h in range(PARTS)] + [finish]

    def together(y_steps, d_steps):
        each = -(-len(d_steps) // len(y_steps))
        for i, step in enumerate(y_steps):
            step()
            for d_step in d_steps[i * each:(i + 1) * each]:
                d_step()

    chip = []
    for i, ks in enumerate(((0,), (1,), (), (2,), (4,), (6,), (3, 5), (7,))):
        j = i % 4
        if 1 in ks:
            arrive(dy_all.at[peer(1)[1]], ys_sem.at[1], yr_sem.at[peer(1)[1]])
        if 2 in ks:
            for n in (2, 4, 6):
                s = peer(n)[1]
                arrive(dy_all.at[s], ys_sem.at[n], yr_sem.at[s])
                sent.append(send(dy_all.at[s], dy_all.at[s], ys_sem.at[n + 1], yr_sem.at[s], 1))
        if 3 in ks:
            for n in (3, 5, 7):
                s = peer(n)[1]
                arrive(dy_all.at[s], ys_sem.at[n], yr_sem.at[s])
        to_chip = i < 4
        together(y_part(peer(2 * j + 1 if to_chip else 2 * j)[1], (y_send if to_chip else y_own).at[j]), [step for k in ks for step in dispatch_dy(peer(k)[1])])
        if to_chip:
            chip.append(send(y_send.at[j], y_chip.at[j], yc_s.at[j], yc_r.at[j], 1))
    for j in (3, 1, 2, 0):
        arrive(y_chip.at[j], yc_s.at[j], yc_r.at[j])
        y_own[j] = y_own[j] + y_chip[j]
        if j == 2:
            far_send(3, 0, 0, 2)
            far_send(3, 1, 1, 4)
            far_send(1, 0, 2, 2)
            far_send(2, 1, 3, 4)
    for k in range(n_src):
        s = peer(k)[1]
        if k:
            sent.append(send(dg_send.at[s], dg_all.at[me], gs_sem.at[k], gr_sem.at[me], k))
        else:
            dg_all[me] = dg_send[s]

    def backward_hidden(e):
        da = _dot(q[e], w2[e % SLOTS].reshape(fh, dm), DIM1).astype(BF).astype(F32)
        uf = u[e].astype(F32)
        vf = v[e].astype(F32)
        sg = jax.nn.sigmoid(uf)
        return (da * vf * sg * (1 + uf * (1 - sg))).astype(BF), (da * (uf * sg)).astype(BF)

    def backward_hiddens(es):
        for e, (du, dv) in [(e, backward_hidden(e)) for e in es]:
            u[e] = du
            v[e] = dv

    def backward_out(e):
        slot = e % SLOTS
        o[e] = (_dot(u[e], w1[slot], DIM1) + _dot(v[e], w3[slot], DIM1)).astype(BF)

    def refill(copies, es):
        for e in es:
            @pl.when(e >= SLOTS)
            def _():
                start(copies(e - SLOTS))

    def ready(copies, es):
        for e in es:
            @pl.when(e < el - SLOTS)
            def _():
                wait(copies(e))

    def down_group(p):
        return [el - 1 - (p * GROUP + i) for i in range(GROUP)]

    def backward(p, _):
        prev, now = down_group(p - 1), down_group(p)
        ready(up, prev)
        for e in now:
            wait(down(e))
        for e in prev:
            backward_out(e)
        backward_hiddens(now)
        refill(up, prev)
        refill(down, now)
        return 0

    for e in down_group(0):
        wait(down(e))
    backward_hiddens(down_group(0))
    refill(down, down_group(0))
    lax.fori_loop(1, groups, backward, 0)
    ready(up, down_group(groups - 1))
    for e in down_group(groups - 1):
        backward_out(e)

    for k in range(1, n_src):
        s = peer(k)[1]
        arrive(dg_all.at[s], gs_sem.at[k], gr_sem.at[s])
    for c in chip:
        c.wait_send()

    def dx_part(s):
        return _dot(onehot_t[s], o[:, rows_of(s), :].reshape(el * ROWS, dm))

    for j in range(4):
        y_send[j] = dx_part(peer(2 * j + 1)[1])
        sent.append(send(y_send.at[j], y_chip.at[j], dc_s.at[j], dc_r.at[j], 1))
    d_own = (dx_here, to_x.at[pl.ds(0, td)], to_y.at[pl.ds(0, td)], to_xy)
    for j in range(4):
        d_own[j][...] = dx_part(peer(2 * j)[1])

    to_y[pl.ds(td, half), :] = far_sum(0, 2, 0)
    to_x[pl.ds(td, half), :] = far_sum(1, 1, 1)
    y_here[pl.ds(0, half), :] = far_sum(2, 0, 0)
    y_here[pl.ds(half, half), :] = far_sum(3, 0, 1)
    dg_out[...] = jnp.sum(dg_all[...], axis=0)

    for j in range(4):
        arrive(y_chip.at[j], dc_s.at[j], dc_r.at[j])
        d_own[j][...] = d_own[j][...] + y_chip[j]

    for c in sent:
        c.wait_send()


def _grad_kernel(xg, q, act, du, dv, dg, dw1, dw3, dw2, dg_out):
    for i in range(xg.shape[0]):
        dw1[i] = _dot(xg[i], du[i], DIM0)
        dw3[i] = _dot(xg[i], dv[i], DIM0)
        dw2[i] = _dot(act[i], q[i], DIM0)
    dg_out[...] = dg[...]


def _finish_kernel(y_here, dx_here, from_x, from_y, from_xy, y, dx):
    td = y.shape[0]
    half = td // 2
    dx[...] = (dx_here[...] + from_x[:td, :] + from_y[:td, :] + from_xy[...]).astype(BF)
    y[:half, :] = (y_here[:half, :] + from_y[td:, :]).astype(BF)
    y[half:, :] = (y_here[half:, :] + from_x[td:, :]).astype(BF)


def solution(mesh):
    ep = ('row', 'col', 'core')
    n_src = mesh.shape['row'] * mesh.shape['col'] * mesh.shape['core']
    tspec = P(('dp',) + ep, None)
    wspec = P(ep, None, None)
    gspec = P(('dp',) + ep, None, None)

    def body(x, route_idx, gates, w1, w3, w2, dy):
        td, top = route_idx.shape
        el, dm, fh = w1.shape
        er = n_src * ROWS
        sds = jax.ShapeDtypeStruct
        vmem = pltpu.VMEM
        dma = pltpu.SemaphoreType.DMA
        block = (td, dm)
        small = (n_src, top, td)
        whole = pl.BlockSpec(memory_space=pltpu.VMEM)
        flops = 2 * el * er * dm * fh * 6
        xg, q, act, du, dv, dg, y_here, dx_here, to_x, to_y, to_xy = pl.pallas_call(
            _core_kernel,
            name='moe_core',
            out_shape=[vmem((el, er, dm), BF), vmem((el, er, dm), BF)] + [vmem((el, er, fh), BF)] * 3
            + [vmem((top, td), F32), vmem(block, F32), vmem(block, F32)]
            + [vmem((td + td // 2, dm), F32)] * 2 + [vmem(block, F32)],
            in_specs=[ANY] * 7,
            out_specs=[whole] * 11,
            scratch_shapes=[
                vmem((n_src,) + block, BF), vmem((n_src,) + block, BF), vmem(small, jnp.int32), vmem(small, F32),
                vmem((el, er, dm), BF),
                vmem((n_src, el * ROWS, td), BF), vmem((n_src, td, el * ROWS), BF), vmem((n_src, 3 * td, el * ROWS), BF),
                vmem((SLOTS, dm, fh), BF), vmem((SLOTS, dm, fh), BF), vmem((SLOTS, fh // er, er, dm), BF),
                vmem((4,) + block, F32), vmem((4,) + block, F32), vmem((4,) + block, F32), vmem((4, td // 2, dm), F32),
                vmem(small, F32), vmem(small, F32),
                dma((4,)), dma((3, SLOTS)), dma((el,)),
                dma((16,)), dma((16,)), dma((8,)), dma((8,)), dma((8,)), dma((8,)), dma((8,)), dma((8,)),
                dma((4,)), dma((4,)), dma((4,)), dma((4,)), dma((4,)), dma((4,)), dma((8,)), dma((8,)),
            ],
            compiler_params=pltpu.CompilerParams(collective_id=0, has_side_effects=True, vmem_limit_bytes=CORE_VMEM << 20),
            cost_estimate=pl.CostEstimate(flops=flops, bytes_accessed=88 << 20, transcendentals=0),
        )(x, dy, route_idx.T, gates.T, w1, w3, w2.reshape(el, fh // er, er, dm))

        def swap(a, k):
            return lax.ppermute(a, ep, [(i, i ^ k) for i in range(n_src)])

        from_xy, from_x, from_y = swap(to_xy, 6), swap(to_x, 2), swap(to_y, 4)
        per = 2
        spec = lambda a, b: pl.BlockSpec((per, a, b), lambda i: (i, 0, 0))
        once = lambda a, b: pl.BlockSpec((a, b), lambda i: (0, 0))

        dw1, dw3, dw2, dg = pl.pallas_call(
            _grad_kernel,
            name='moe_grad',
            grid=(el // per,),
            out_shape=[sds((el, dm, fh), F32), sds((el, dm, fh), F32), sds((el, fh, dm), F32), sds((top, td), F32)],
            in_specs=[spec(er, dm), spec(er, dm), spec(er, fh), spec(er, fh), spec(er, fh), once(top, td)],
            out_specs=[spec(dm, fh), spec(dm, fh), spec(fh, dm), once(top, td)],
            compiler_params=pltpu.CompilerParams(vmem_limit_bytes=GRAD_VMEM << 20),
            cost_estimate=pl.CostEstimate(flops=2 * el * er * dm * fh * 3, bytes_accessed=90 << 20, transcendentals=0),
        )(xg, q, act, du, dv, dg)
        y, dx = pl.pallas_call(
            _finish_kernel,
            name='moe_finish',
            out_shape=[sds(block, BF), sds(block, BF)],
            in_specs=[whole] * 5,
            out_specs=[whole] * 2,
            compiler_params=pltpu.CompilerParams(vmem_limit_bytes=FINISH_VMEM << 20),
        )(y_here, dx_here, from_x, from_y, from_xy)
        return y, dx, dg.T, dw1, dw3, dw2

    return jax.shard_map(body, mesh=mesh, in_specs=(tspec, tspec, tspec, wspec, wspec, wspec, tspec),
                         out_specs=(tspec, tspec, tspec, gspec, gspec, gspec), check_vma=False)
```
